512 devices in a mesh: lat: 32 (over y, z_hi, core), lev: 16 (over x, z_lo).
Axes of the slice: x: 4, y: 8, z: 8 (z_hi: 2, z_lo: 4; z = z_hi * 4 + z_lo), core: 2. Of those that a mesh axis runs over, the one named last changes fastest.
Arguments:
- tracer: float32 [32, 640, 1280], P('lev', 'lat'), may hold values from -6 to 6
- offsets: int32 [2, 640, 1280], P(None, 'lat'), may hold values from -3 to 3
- stencil: float32 [7, 7], replicated, may hold values from -0.6 to 0.6
- assign: int32 [640], replicated, may hold values from 0 to 639, as said below
- legendre: bfloat16 [640, 2, 320, 320], P('lat', None, 'lev'), may hold values from -0.3125 to 0.3125
- damping: float32 [32], replicated, may hold values from 0.5 to 8
- vert_vecs: float32 [32, 32], replicated, may hold values from -1 to 1
- vert_inv: float32 [32, 32], replicated, may hold values from -1 to 1
Outputs:
- tracer_new: float32 [32, 640, 1280], P('lev', 'lat')
- spectral_new: float32 [640, 2, 320, 64], P('lat', None, 'lev')
The draws below stay inside these ranges and needn't reach their ends.
Inputs may be any that keep to these rules, and one draw needn't show every extreme that they name: `assign`: a permutation of 0 to 639 in which slots 2 u and 2 u + 1 hold the wavenumbers m and 639 - m.
All inputs are finite; a program needn't handle non-finite values.
Results may differ from the reference program's by a relative error of at most 0.0036.
Values may be sent and summed in bfloat16 or wider, within the bound.
No kernel may reach another device: no remote copies, remote signals or barrier semaphores. Data moves between devices by JAX's collectives and lax.ppermute only.
A program may use at most 128 MiB of HBM per device.

```python
import math
import jax
import jax.numpy as jnp
from jax import lax

NLON = 1280
NLAT = 640
M = 640
NLEV = 32
HALF_DEG = 320
HALF_LAT = 320


def draw_assign(key, part):
    paired = jax.random.permutation(jax.random.fold_in(key, 7), M // 2).astype(jnp.int32)
    return jnp.stack([paired, M - 1 - paired], axis=1).reshape(M)


def place_ends(result, stream_key, low, largest):
    longest = result.shape.index(max(result.shape))
    spots = []
    for shift in (0, 1):
        where = [jax.random.randint(jax.random.fold_in(stream_key, axis), (), 0, length) for axis, length in enumerate(result.shape)]
        where[longest] = (where[longest] + shift) % result.shape[longest]
        spots.append(tuple(where))
    return result.at[spots[0]].set(low).at[spots[1]].set(largest)


def level_of(key, dims, shards, least, top_value):
    level = 1.0
    for dim, shards_of in shards:
        steps = jax.random.uniform(jax.random.fold_in(jax.random.fold_in(key, 6), dim), (shards_of,), jnp.float32, least / len(shards), top_value / len(shards))
        level = level * jnp.repeat(jnp.exp(steps), dims[dim] // shards_of).reshape((-1,) + (1,) * (len(dims) - 1 - dim))
    return level


def scatter_about(stream_key, shape, deviation, limit, split=(), kind=jnp.bfloat16):
    level = level_of(stream_key, shape, split, -0.22, 0.18) if split else 1.0
    values = jax.random.normal(stream_key, shape, jnp.float32) * deviation * level
    return jnp.minimum(jnp.maximum(values, -limit), limit).astype(kind)


def setup_inputs(seed: int = 0) -> dict:
    streams_of = jax.random.split(jax.random.key(seed), 9)
    tracer = scatter_about(streams_of[0], (NLEV, NLAT, NLON), 1.0, 6.0, ((0, 16), (1, 32)), jnp.float32)
    offsets = place_ends(jax.random.randint(streams_of[1], (2, NLAT, NLON), -3, 4), jax.random.fold_in(streams_of[1], 1), -3, 3).astype(jnp.int32)
    stencil = scatter_about(streams_of[2], (7, 7), 0.15, 0.6, (), jnp.float32)
    assign = draw_assign(jax.random.fold_in(streams_of[8], 71), 0)
    legendre = scatter_about(streams_of[4], (M, 2, HALF_DEG, HALF_LAT), HALF_LAT ** -0.5, 0.3125, ((0, 32), (2, 16)))
    damping = jnp.clip(jnp.exp(jax.random.uniform(streams_of[5], (NLEV,), jnp.float32, math.log(0.5), math.log(8.0))), 0.5, 8.0)
    vert_vecs = scatter_about(streams_of[6], (NLEV, NLEV), NLEV ** -0.5, 1.0, (), jnp.float32)
    vert_inv = scatter_about(streams_of[7], (NLEV, NLEV), NLEV ** -0.5, 1.0, (), jnp.float32)
    return dict(tracer=tracer, offsets=offsets, stencil=stencil, assign=assign, legendre=legendre, damping=damping, vert_vecs=vert_vecs, vert_inv=vert_inv)


EXACT = lax.Precision.HIGHEST

def transport(padded, offsets, stencil):
    row_count = offsets.shape[1]
    summed = jnp.zeros((padded.shape[0], row_count, padded.shape[2]), jnp.float32)
    for row_step in range(-3, 4):
        band_rows = padded[:, 3 + row_step:3 + row_step + row_count, :]
        for col_step in range(-3, 4):
            shifted = jnp.roll(band_rows, -col_step, axis=2)
            picked = jnp.logical_and(offsets[0] == row_step, offsets[1] == col_step).astype(jnp.float32)
            summed = summed + (stencil[row_step + 3, col_step + 3] + picked)[None, :, :] * shifted
    return summed

def wave_angles(assign, lon_cells):
    longitudes = jnp.arange(lon_cells, dtype=jnp.int32)
    phase_index = longitudes[:, None] * assign[None, :].astype(jnp.int32) % lon_cells
    angles = phase_index.astype(jnp.float32) * (2.0 * math.pi / lon_cells)
    return (angles, 1.0 / math.sqrt(lon_cells))

def forward_table(assign, lon_cells):
    angles, norm_scale = wave_angles(assign, lon_cells)
    return jnp.stack([jnp.cos(angles) * norm_scale, -jnp.sin(angles) * norm_scale], axis=2)

def inverse_table(assign, lon_cells):
    angles, norm_scale = wave_angles(assign, lon_cells)
    weights = jnp.where(assign == 0, 1.0, 2.0).astype(jnp.float32) * norm_scale
    cosines = jnp.cos(angles).T * weights[:, None]
    sines = -jnp.sin(angles).T * weights[:, None]
    return jnp.stack([cosines, sines], axis=1)

def split_hemispheres(fourier):
    half_lat = fourier.shape[-1] // 2
    north_half = fourier[..., :half_lat]
    south_half = fourier[..., ::-1][..., :half_lat]
    return jnp.stack([north_half + south_half, north_half - south_half], axis=1).astype(jnp.bfloat16)

def vertical(spectra, my_waves, first_degree, damping, vert_vecs, vert_inv):
    degree_span = spectra.shape[2]
    degrees = first_degree + jnp.arange(degree_span, dtype=jnp.int32)
    parity = jnp.arange(2, dtype=jnp.int32)
    degree_n = my_waves.astype(jnp.int32)[:, None, None] + 2 * degrees[None, None, :] + parity[None, :, None]
    inside = (degree_n <= M - 1).astype(jnp.float32)
    forcing = spectra * inside[:, :, :, None, None]
    modal = jnp.einsum('kq,rpicq->rpick', vert_inv, forcing, precision=EXACT)
    scaled_n = degree_n.astype(jnp.float32)
    growth = scaled_n * (scaled_n + 1.0) / float(M * M)
    denominator = 1.0 + growth[:, :, :, None, None] * damping[None, None, None, None, :]
    modal = modal / denominator
    return jnp.einsum('kq,rpicq->rpick', vert_vecs, modal, precision=EXACT)

def reference(tracer, offsets, stencil, assign, legendre, damping, vert_vecs, vert_inv):
    lon_cells = tracer.shape[2]
    padded = jnp.pad(tracer, ((0, 0), (3, 3), (0, 0)))
    advected = transport(padded, offsets, stencil)
    fourier = jnp.einsum('lij,jrc->rcli', advected, forward_table(assign, lon_cells), precision=EXACT)
    hemispheres = split_hemispheres(fourier)

    def forward_slot(pair):
        table_slot, hemi_slot = pair
        return jnp.einsum('pij,pclj->picl', table_slot.astype(jnp.float32), hemi_slot.astype(jnp.float32))
    spectra = lax.map(forward_slot, (legendre, hemispheres))
    solved = vertical(spectra, assign, 0, damping, vert_vecs, vert_inv)
    packed = solved.astype(jnp.bfloat16)

    def inverse_slot(pair):
        table_slot, packed_slot = pair
        return jnp.einsum('pij,picl->lpcj', table_slot.astype(jnp.float32), packed_slot.astype(jnp.float32))
    back_terms = lax.map(inverse_slot, (legendre, packed))
    north_half = back_terms[:, :, 0] + back_terms[:, :, 1]
    south_half = back_terms[:, :, 0] - back_terms[:, :, 1]
    zonal = jnp.concatenate([north_half, south_half[..., ::-1]], axis=-1)
    tracer_new = jnp.einsum('rlci,rcj->lij', zonal, inverse_table(assign, lon_cells), precision=EXACT)
    spectral_new = solved.reshape(solved.shape[0], 2, solved.shape[2], 2 * solved.shape[4])
    return (tracer_new, spectral_new)
```

```python
import functools
import math

import jax
import jax.numpy as jnp
from jax import lax
from jax.experimental import pallas as pl
from jax.experimental.pallas import tpu as pltpu
from jax.sharding import PartitionSpec as P

INTERPRET = False
N_LAT, N_LEV = 32, 16
N_DEV = N_LAT * N_LEV
M = 640
NLON, HALF_LON = 1280, 640
ROWS = 20
LV = 2
NLEV = 32
QB = 40
QP = N_LEV * QB
HL = 320
SLOTS = 20
MSG = LV * ROWS
F32, BF16 = jnp.float32, jnp.bfloat16
NT = (((1,), (1,)), ((), ()))
NN = (((1,), (0,)), ((), ()))
HIGH = lax.Precision.HIGHEST


def first_rc(b):
    return (5 * b) >> 1


def call(kernel, out_shape, in_specs, scratch, name, flops=10**7):
    many = isinstance(out_shape, (tuple, list))
    vm = pl.BlockSpec(memory_space=pltpu.VMEM)
    return pl.pallas_call(
        kernel,
        out_shape=out_shape,
        in_specs=in_specs,
        out_specs=[vm] * len(out_shape) if many else vm,
        scratch_shapes=scratch,
        name=name,
        interpret=INTERPRET,
        cost_estimate=pl.CostEstimate(flops=flops, bytes_accessed=10**6, transcendentals=0),
    )


VM = pl.BlockSpec(memory_space=pltpu.VMEM)
ANY = pl.BlockSpec(memory_space=pl.ANY)
SM = pl.BlockSpec(memory_space=pltpu.SMEM)


def cos_sin(phase):
    quad = jnp.floor((phase + 160.5) * (1.0 / 320.0))
    x = (phase - 320.0 * quad) * (2.0 * math.pi / NLON)
    z = x * x
    s = x * (1.0 + z * (-1.6666654611e-1 + z * (8.3321608736e-3 - z * 1.9515295891e-4)))
    c = 1.0 - 0.5 * z + z * z * (
        4.166664568298827e-2 + z * (-1.388731625493765e-3 + z * 2.443315711809948e-5)
    )
    odd = jnp.logical_or(quad == 1.0, quad == 3.0)
    c, s = jnp.where(odd, s, c), jnp.where(odd, c, s)
    c = jnp.where(jnp.logical_or(quad == 1.0, quad == 2.0), -c, c)
    s = jnp.where(jnp.logical_or(quad == 2.0, quad == 3.0), -s, s)
    return c, s


def wrapped(count):
    return count - NLON * jnp.floor((count + 0.5) * (1.0 / NLON))


CHUNK = 64


def tables_kernel(assign_ref, t_ref, even_ref, weight_ref):
    slots = lax.broadcasted_iota(jnp.int32, (CHUNK, M), 1)
    lane = lax.broadcasted_iota(jnp.int32, (CHUNK, 128), 1)
    lane_f = lane.astype(F32)
    assign = assign_ref[...]

    def step(i, carry):
        r0 = pl.multiple_of(i * CHUNK, CHUNK)
        d = r0 + lax.broadcasted_iota(jnp.int32, (CHUNK, 1), 0)
        rc0 = ((d & 15) * 5) >> 1
        evens, weights, waves = [], [], []
        for j in range(3):
            slot = (d >> 4) * SLOTS + ((rc0 + j) >> 1)
            waves.append(jnp.sum(jnp.where(slots == slot, assign, 0.0), axis=1, keepdims=True))
            evens.append(jnp.where(waves[j] == 2.0 * jnp.floor(waves[j] * 0.5), 1.0, 0.0))
            weights.append(jnp.where(waves[j] == 0.0, 1.0, 2.0))
        packed = jnp.where(lane == 0, waves[0], jnp.where(lane == 1, waves[1], waves[2]))
        turn_c, turn_s = cos_sin(wrapped(packed * 128.0))
        for j in range(3):
            quarter = jnp.where(((rc0 + j) & 1) == 1, 320.0, 0.0)
            c, s = cos_sin(wrapped(waves[j] * lane_f + quarter))
            c = c * (1.0 / math.sqrt(NLON))
            s = s * (1.0 / math.sqrt(NLON))
            cd, sd = turn_c[:, j : j + 1], turn_s[:, j : j + 1]
            for block in range(5):
                high = c.astype(BF16)
                t_ref[j, pl.ds(r0, CHUNK), 128 * block : 128 * block + 128] = high
                t_ref[
                    j, pl.ds(r0, CHUNK), HALF_LON + 128 * block : HALF_LON + 128 * block + 128
                ] = (c - high.astype(F32)).astype(BF16)
                if block < 4:
                    c, s = c * cd - s * sd, s * cd + c * sd
        even_ref[pl.ds(r0, CHUNK), :] = jnp.where(
            lane < MSG, evens[0], jnp.where(lane < 2 * MSG, evens[1], evens[2])
        )
        weight_ref[pl.ds(r0, CHUNK), :] = jnp.where(
            lane < MSG, weights[0], jnp.where(lane < 2 * MSG, weights[1], weights[2])
        )
        return carry

    lax.fori_loop(0, N_DEV // CHUNK, step, 0)


def tables(assign):
    return call(
        tables_kernel,
        (
            jax.ShapeDtypeStruct((3, N_DEV, NLON), BF16),
            jax.ShapeDtypeStruct((N_DEV, 128), F32),
            jax.ShapeDtypeStruct((N_DEV, 128), F32),
        ),
        [VM],
        [],
        "tables",
    )(assign.astype(F32).reshape(1, M))


def forward_kernel(
    stencil_ref,
    tracer_ref,
    north_ref,
    south_ref,
    off_ref,
    t_any,
    even_ref,
    out_ref,
    pad,
    rolled,
    codes,
    adv,
    fe,
    fo,
    t_ref,
    t_sem,
):
    fetch = pltpu.make_async_copy(t_any, t_ref, t_sem)
    fetch.start()
    pad[...] = jnp.zeros((64, NLON), F32)
    for i in range(3):
        pad[2 + 2 * i : 4 + 2 * i, :] = north_ref[i]
        pad[48 + 2 * i : 50 + 2 * i, :] = south_ref[i]
    for i in range(ROWS):
        pad[8 + 2 * i : 10 + 2 * i, :] = tracer_ref[i]
        codes[2 * i : 2 * i + 2, :] = off_ref[i]
    for bi in range(7):
        shift = (3 - bi) % NLON
        rolled[bi] = pltpu.roll(pad[...], shift, 1) if shift else pad[...]

    first = (lax.broadcasted_iota(jnp.int32, (2 * ROWS, 128), 0) & 1) == 0

    def chunk(ci, carry):
        l0 = pl.multiple_of(ci * 128, 128)
        value = codes[:, pl.ds(l0, 128)]
        part = jnp.where(first, value * 7, value)
        code = part + jnp.where(first, jnp.roll(part, -1, 0), jnp.roll(part, 1, 0))
        acc = jnp.zeros((2 * ROWS, 128), F32)
        for ai in range(7):
            for bi in range(7):
                s = stencil_ref[ai, bi]
                w = jnp.where(code == (ai - 3) * 7 + (bi - 3), s + 1.0, s)
                acc = acc + w * rolled[bi, 2 + 2 * ai : 42 + 2 * ai, pl.ds(l0, 128)]
        adv[ci] = acc
        return carry

    lax.fori_loop(0, NLON // 128, chunk, 0)
    levels = [
        jnp.concatenate([every_other(adv, ci, k) for ci in range(NLON // 128)], axis=1) for k in range(LV)
    ]
    x = jnp.concatenate(
        [v[:, :HALF_LON] + v[:, HALF_LON:] for v in levels] + [v[:, :HALF_LON] - v[:, HALF_LON:] for v in levels], axis=0
    )
    high = x.astype(BF16)
    low = (x - high.astype(F32)).astype(BF16)
    right = jnp.concatenate(
        [
            jnp.concatenate([high, high], axis=1),
            jnp.concatenate([low, jnp.zeros_like(low)], axis=1),
        ],
        axis=0,
    )
    fe[...] = jnp.zeros((N_DEV, 128), F32)
    fo[...] = jnp.zeros((N_DEV, 128), F32)
    fetch.wait()
    for j in range(3):
        prod = lax.dot_general(t_ref[j], right, NT, preferred_element_type=F32)
        fe[:, MSG * j : MSG * (j + 1)] = prod[:, 0:MSG] + prod[:, 2 * MSG : 3 * MSG]
        fo[:, MSG * j : MSG * (j + 1)] = prod[:, MSG : 2 * MSG] + prod[:, 3 * MSG : 4 * MSG]
    out_ref[...] = jnp.where(even_ref[...] > 0.5, fe[...], fo[...])


def every_other(ref, ci, k):
    return ref[ci][k::2] if INTERPRET else ref[ci, pl.ds(k, ROWS, 2), :]


def forward(stencil, tracer, north, south, offsets, table, even):
    return call(
        forward_kernel,
        jax.ShapeDtypeStruct((N_DEV, 128), F32),
        [SM, VM, VM, VM, VM, ANY, VM],
        [
            pltpu.VMEM((64, NLON), F32),
            pltpu.VMEM((7, 64, NLON), F32),
            pltpu.VMEM((2 * ROWS, NLON), jnp.int32),
            pltpu.VMEM((NLON // 128, 2 * ROWS, 128), F32),
            pltpu.VMEM((N_DEV, 128), F32),
            pltpu.VMEM((N_DEV, 128), F32),
            pltpu.VMEM((3, N_DEV, NLON), BF16),
            pltpu.SemaphoreType.DMA,
        ],
        "forward",
        10**9,
    )(stencil, tracer, north, south, offsets, table, even)


def mirror_matrix():
    src = lax.broadcasted_iota(jnp.int32, (128, 128), 0)
    dst = lax.broadcasted_iota(jnp.int32, (128, 128), 1)
    hit = jnp.zeros((128, 128), jnp.bool_)
    for g in range(6):
        hit = jnp.logical_or(
            hit, jnp.logical_and(jnp.logical_and(dst >= 20 * g, dst < 20 * g + 20), src + dst == 40 * g + 19)
        )
    return hit.astype(F32)


def spectral_kernel(
    info_ref, msg_ref, table_ref, damping_ref, inv_ref, vec_ref, vecp_ref, out_ref, spec_ref, nbuf, sbuf, flip, zn, zs, sall
):
    mirror = mirror_matrix()
    half = N_DEV // 2
    flip[...] = lax.dot_general(msg_ref[half:, :], mirror, NN, precision=HIGH, preferred_element_type=F32)
    for a in range(N_LAT // 2):
        top = msg_ref[16 * a : 16 * a + 16, :]
        low = flip[16 * (15 - a) : 16 * (15 - a) + 16, :]
        for j in range(3):
            for k in range(LV):
                lane = MSG * j + ROWS * k
                nbuf[j, 16 * k : 16 * k + 16, ROWS * a : ROWS * a + ROWS] = top[:, lane : lane + ROWS]
                sbuf[j, 16 * k : 16 * k + 16, ROWS * a : ROWS * a + ROWS] = low[:, lane : lane + ROWS]
    parity = info_ref[2]
    lev_odd = info_ref[3]
    lane = lax.broadcasted_iota(jnp.int32, (32, QP), 1)
    odd = lane & 1
    damp = damping_ref[...]
    matrix = [table_ref[0], table_ref[parity], table_ref[1]]
    degree = [
        lane + (info_ref[0] if j == 0 else (info_ref[1] if j == 2 else jnp.where(parity == 1, info_ref[1], info_ref[0])))
        for j in range(3)
    ]
    for j in range(3):
        north, south = nbuf[j], sbuf[j]
        hemi = jnp.concatenate([north + south, north - south], axis=0).astype(BF16)
        prod = lax.dot_general(hemi, matrix[j], NT, preferred_element_type=F32)
        keep = degree[j] <= M - 1
        if j == 0:
            keep = jnp.logical_and(keep, odd >= lev_odd)
        if j == 2:
            keep = jnp.logical_and(keep, odd <= lev_odd)
        sall[32 * j : 32 * j + 32, :] = jnp.where(keep, jnp.where(odd == 1, prod[32:], prod[:32]), 0.0)
    modal = lax.dot_general(inv_ref[...], sall[...], NN, precision=HIGH, preferred_element_type=F32)
    for j in range(3):
        n = degree[j].astype(F32)
        growth = n * (n + 1.0) / float(M * M)
        sall[32 * j : 32 * j + 32, :] = modal[32 * j : 32 * j + 32, :] / (1.0 + growth * damp)
    modal = sall[...]
    solved = lax.dot_general(vec_ref[...], modal, NN, precision=HIGH, preferred_element_type=F32).T
    for b in range(N_LEV):
        spec_ref[b] = solved[QB * b : QB * b + QB].astype(BF16)
    sall[...] = lax.dot_general(vecp_ref[...], modal, NN, precision=HIGH, preferred_element_type=F32)
    for j in range(3):
        mine = sall[32 * j : 32 * j + 32, :]
        left = jnp.concatenate([mine, jnp.where(odd == 1, -mine, mine)], axis=0).astype(BF16)
        both = lax.dot_general(left, matrix[j], NN, preferred_element_type=F32)
        zn[j] = both[:32]
        zs[j] = both[32:]
    out_ref[...] = jnp.zeros((N_DEV, 128), F32)
    flip[...] = jnp.zeros((half, 128), F32)
    for a in range(N_LAT // 2):
        for j in range(3):
            for k in range(LV):
                lane = MSG * j + ROWS * k
                out_ref[16 * a : 16 * a + 16, lane : lane + ROWS] = zn[j, 16 * k : 16 * k + 16, ROWS * a : ROWS * a + ROWS]
                flip[16 * (15 - a) : 16 * (15 - a) + 16, lane : lane + ROWS] = zs[
                    j, 16 * k : 16 * k + 16, ROWS * a : ROWS * a + ROWS
                ]
    out_ref[half:, :] = lax.dot_general(flip[...], mirror, NN, precision=HIGH, preferred_element_type=F32)


def spectral(info, msgs, table, damping, inv, vec, vecp):
    return call(
        spectral_kernel,
        (jax.ShapeDtypeStruct((N_DEV, 128), F32), jax.ShapeDtypeStruct((N_LEV, QB, 96), BF16)),
        [SM, VM, VM, VM, VM, VM, VM],
        [
            pltpu.VMEM((3, 32, HL), F32),
            pltpu.VMEM((3, 32, HL), F32),
            pltpu.VMEM((N_DEV // 2, 128), F32),
            pltpu.VMEM((3, 32, HL), F32),
            pltpu.VMEM((3, 32, HL), F32),
            pltpu.VMEM((96, QP), F32),
        ],
        "spectral",
        10**9,
    )(info, msgs, table, damping, inv, vec, vecp)


def inverse_kernel(msg_ref, t_any, even_ref, weight_ref, out_ref, t_ref, t_sem):
    fetch = pltpu.make_async_copy(t_any.at[:, :, pl.ds(0, HALF_LON)], t_ref, t_sem)
    fetch.start()
    lane = lax.broadcasted_iota(jnp.int32, (N_DEV, 128), 1)
    scaled = jnp.where(lane < 3 * MSG, msg_ref[...] * weight_ref[...], 0.0)
    even = (scaled * even_ref[...]).T
    odd = (scaled * (1.0 - even_ref[...])).T
    total = jnp.zeros((2 * MSG, HALF_LON), F32)
    fetch.wait()
    for j in range(3):
        left = jnp.concatenate([even[MSG * j : MSG * (j + 1)], odd[MSG * j : MSG * (j + 1)]], axis=0).astype(BF16)
        total = total + lax.dot_general(left, t_ref[j], NN, preferred_element_type=F32)
    near = total[:MSG] + total[MSG:]
    far = total[:MSG] - total[MSG:]
    for k in range(LV):
        out_ref[:, k, :HALF_LON] = near[ROWS * k : ROWS * (k + 1)]
        out_ref[:, k, HALF_LON:] = far[ROWS * k : ROWS * (k + 1)]


def inverse(msgs, table, even, weight):
    return call(
        inverse_kernel,
        jax.ShapeDtypeStruct((ROWS, LV, NLON), F32),
        [VM, ANY, VM, VM],
        [pltpu.VMEM((3, N_DEV, HALF_LON), BF16), pltpu.SemaphoreType.DMA],
        "inverse",
        10**8,
    )(msgs, table, even, weight)


def place_kernel(spec_ref, out_ref):
    for slot in range(SLOTS):
        for c in range(2):
            w, o = divmod(2 * slot + c, 5)
            parts = []
            if o <= 2:
                parts.append((2 * w, o))
            if o >= 2:
                parts.append((2 * w + 1, o - 2))
            value = sum(spec_ref[b, :, 32 * j : 32 * j + 32].astype(F32) for b, j in parts)
            out_ref[slot, :, 32 * c : 32 * c + 32] = value


def place(spec):
    return call(place_kernel, jax.ShapeDtypeStruct((SLOTS, QB, 64), F32), [VM], [], "place", 10**6)(spec)


def by_block(matrix):
    return jnp.kron(jnp.eye(3, dtype=F32), matrix)


def level_order(value, axis):
    shape = value.shape
    split = shape[:axis] + (16, 2) + shape[axis + 1 :]
    return jnp.swapaxes(value.reshape(split), axis, axis + 1).reshape(shape)


def send_kernel(table_ref, out_ref, sems):
    copies = []
    for b in range(N_LEV):
        first = first_rc(b) >> 1
        copies.append(pltpu.make_async_copy(table_ref.at[pl.ds(first, 2)], out_ref.at[b], sems.at[b]))
    for copy in copies:
        copy.start()
    for copy in copies:
        copy.wait()


def send_tables(legendre):
    return pl.pallas_call(
        send_kernel,
        out_shape=jax.ShapeDtypeStruct((N_LEV, 2, 20, 2, HL), BF16),
        in_specs=[ANY],
        out_specs=ANY,
        scratch_shapes=[pltpu.SemaphoreType.DMA((N_LEV,))],
        name="send_tables",
        interpret=INTERPRET,
        cost_estimate=pl.CostEstimate(flops=10**6, bytes_accessed=2 * 10**6, transcendentals=0),
    )(jnp.swapaxes(legendre, 1, 2))


def received_tables(got):
    return jnp.swapaxes(got, 0, 1).reshape(2, QP, HL)


def exchange(value, axes):
    return lax.all_to_all(value, axes, split_axis=0, concat_axis=0, tiled=True)


def on_device(tracer, offsets, stencil, assign, legendre, damping, vert_vecs, vert_inv):
    up = [(i, i + 1) for i in range(N_LAT - 1)]
    down = [(i + 1, i) for i in range(N_LAT - 1)]
    rows = jnp.swapaxes(tracer, 0, 1)
    north = lax.ppermute(rows[ROWS - 3 :], "lat", up)
    south = lax.ppermute(rows[:3], "lat", down)
    table, even, weight = tables(assign)
    with jax.named_scope("tabx"):
        matrices = exchange(send_tables(legendre), "lev")
    matrices = received_tables(matrices)
    msgs = forward(stencil, rows, north, south, jnp.swapaxes(offsets, 0, 1), table, even)
    with jax.named_scope("fwdx"):
        got = exchange(msgs.reshape(N_DEV, 1, 128), ("lat", "lev")).reshape(N_DEV, 128)
    lev = lax.axis_index("lev")
    rc0 = (5 * lev) >> 1
    waves = lax.dynamic_slice_in_dim(assign, lax.axis_index("lat") * SLOTS + (rc0 >> 1), 2)
    info = jnp.concatenate([waves, jnp.stack([rc0 & 1, lev & 1])]).astype(jnp.int32)
    back, spec = spectral(
        info,
        got,
        matrices,
        damping.reshape(32, 1),
        by_block(level_order(vert_inv, 1)),
        by_block(vert_vecs),
        by_block(level_order(vert_vecs, 0)),
    )
    with jax.named_scope("bwdx"):
        home = exchange(back.reshape(N_DEV, 1, 128), ("lat", "lev")).reshape(N_DEV, 128)
    with jax.named_scope("specx"):
        spec = exchange(spec, "lev")
    tracer_new = inverse(home, table, even, weight)
    spectral_new = place(spec).reshape(SLOTS, 20, 2, 64)
    return jnp.swapaxes(tracer_new, 0, 1), jnp.swapaxes(spectral_new, 1, 2)


def solution(mesh):
    placed = (
        P("lev", "lat", None),
        P(None, "lat", None),
        P(),
        P(),
        P("lat", None, "lev", None),
        P(),
        P(),
        P(),
    )
    return jax.shard_map(
        on_device,
        mesh=mesh,
        in_specs=placed,
        out_specs=(P("lev", "lat", None), P("lat", None, "lev", None)),
        check_vma=False,
    )
```

```python
import functools
import math

import jax
import jax.numpy as jnp
from jax import lax
from jax.experimental import pallas as pl
from jax.experimental.pallas import tpu as pltpu
from jax.sharding import PartitionSpec as P

INTERPRET = False
N_LAT, N_LEV = 32, 16
N_DEV = N_LAT * N_LEV
M = 640
NLON, HALF_LON = 1280, 640
ROWS = 20
LV = 2
NLEV = 32
QB = 40
QP = N_LEV * QB
HL = 320
SLOTS = 20
MSG = LV * ROWS
F32, BF16 = jnp.float32, jnp.bfloat16
NT = (((1,), (1,)), ((), ()))
NN = (((1,), (0,)), ((), ()))
HIGH = lax.Precision.HIGHEST


def own_slot(b):
    return 5 * (b >> 2) + (b & 3)


def shared_slot(b):
    return 5 * (b >> 2) + 4


def call(kernel, out_shape, in_specs, scratch, name, flops=10**7):
    many = isinstance(out_shape, (tuple, list))
    vm = pl.BlockSpec(memory_space=pltpu.VMEM)
    return pl.pallas_call(
        kernel,
        out_shape=out_shape,
        in_specs=in_specs,
        out_specs=[vm] * len(out_shape) if many else vm,
        scratch_shapes=scratch,
        name=name,
        interpret=INTERPRET,
        cost_estimate=pl.CostEstimate(flops=flops, bytes_accessed=10**6, transcendentals=0),
    )


VM = pl.BlockSpec(memory_space=pltpu.VMEM)
ANY = pl.BlockSpec(memory_space=pl.ANY)
SM = pl.BlockSpec(memory_space=pltpu.SMEM)


def cos_sin(phase):
    quad = jnp.floor((phase + 160.5) * (1.0 / 320.0))
    x = (phase - 320.0 * quad) * (2.0 * math.pi / NLON)
    z = x * x
    s = x * (1.0 + z * (-1.6666654611e-1 + z * (8.3321608736e-3 - z * 1.9515295891e-4)))
    c = 1.0 - 0.5 * z + z * z * (
        4.166664568298827e-2 + z * (-1.388731625493765e-3 + z * 2.443315711809948e-5)
    )
    odd = jnp.logical_or(quad == 1.0, quad == 3.0)
    c, s = jnp.where(odd, s, c), jnp.where(odd, c, s)
    c = jnp.where(jnp.logical_or(quad == 1.0, quad == 2.0), -c, c)
    s = jnp.where(jnp.logical_or(quad == 2.0, quad == 3.0), -s, s)
    return c, s


def wrapped(count):
    return count - NLON * jnp.floor((count + 0.5) * (1.0 / NLON))


CHUNK = 64


def tables_kernel(assign_ref, t_ref, even_ref, weight_ref):
    slots = lax.broadcasted_iota(jnp.int32, (CHUNK, M), 1)
    lane = lax.broadcasted_iota(jnp.int32, (CHUNK, 128), 1)
    lane_f = lane.astype(F32)
    assign = assign_ref[...]

    def step(i, carry):
        r0 = pl.multiple_of(i * CHUNK, CHUNK)
        d = r0 + lax.broadcasted_iota(jnp.int32, (CHUNK, 1), 0)
        lev = d & 15
        waves, evens, weights = [], [], []
        for slot in (own_slot(lev), shared_slot(lev)):
            wave = jnp.sum(jnp.where(slots == (d >> 4) * SLOTS + slot, assign, 0.0), axis=1, keepdims=True)
            waves.append(wave)
            evens.append(jnp.where(wave == 2.0 * jnp.floor(wave * 0.5), 1.0, 0.0))
            weights.append(jnp.where(wave == 0.0, 1.0, 2.0))
        turn_c, turn_s = cos_sin(wrapped(jnp.where(lane == 0, waves[0], waves[1]) * 128.0))

        def put(j, block, value):
            high = value.astype(BF16)
            t_ref[j, pl.ds(r0, CHUNK), 128 * block : 128 * block + 128] = high
            low = (value - high.astype(F32)).astype(BF16)
            t_ref[j, pl.ds(r0, CHUNK), HALF_LON + 128 * block : HALF_LON + 128 * block + 128] = low

        for u in range(2):
            start = wrapped(waves[u] * lane_f + (jnp.where((lev & 2) == 2, 320.0, 0.0) if u else 0.0))
            c, s = cos_sin(start)
            c = c * (1.0 / math.sqrt(NLON))
            s = s * (1.0 / math.sqrt(NLON))
            cd, sd = turn_c[:, u : u + 1], turn_s[:, u : u + 1]
            for block in range(5):
                put(2 * u, block, c)
                if u == 0:
                    put(1, block, -s)
                if block < 4:
                    c, s = c * cd - s * sd, s * cd + c * sd
        even_ref[pl.ds(r0, CHUNK), :] = jnp.where(
            lane < 2 * MSG, evens[0], evens[1]
        )
        weight_ref[pl.ds(r0, CHUNK), :] = jnp.where(
            lane < 2 * MSG, weights[0], weights[1]
        )
        return carry

    lax.fori_loop(0, N_DEV // CHUNK, step, 0)


def tables(assign):
    return call(
        tables_kernel,
        (
            jax.ShapeDtypeStruct((3, N_DEV, NLON), BF16),
            jax.ShapeDtypeStruct((N_DEV, 128), F32),
            jax.ShapeDtypeStruct((N_DEV, 128), F32),
        ),
        [VM],
        [],
        "tables",
    )(assign.astype(F32).reshape(1, M))


def forward_kernel(
    stencil_ref,
    tracer_ref,
    north_ref,
    south_ref,
    off_ref,
    t_any,
    even_ref,
    out_ref,
    pad,
    rolled,
    codes,
    adv,
    fe,
    fo,
    t_ref,
    t_sem,
):
    fetch = pltpu.make_async_copy(t_any, t_ref, t_sem)
    fetch.start()
    pad[...] = jnp.zeros((64, NLON), F32)
    for i in range(3):
        pad[2 + 2 * i : 4 + 2 * i, :] = north_ref[i]
        pad[48 + 2 * i : 50 + 2 * i, :] = south_ref[i]
    for i in range(ROWS):
        pad[8 + 2 * i : 10 + 2 * i, :] = tracer_ref[i]
        codes[2 * i : 2 * i + 2, :] = off_ref[i]
    for bi in range(7):
        shift = (3 - bi) % NLON
        rolled[bi] = pltpu.roll(pad[...], shift, 1) if shift else pad[...]

    first = (lax.broadcasted_iota(jnp.int32, (2 * ROWS, 128), 0) & 1) == 0

    def chunk(ci, carry):
        l0 = pl.multiple_of(ci * 128, 128)
        value = codes[:, pl.ds(l0, 128)]
        part = jnp.where(first, value * 7, value)
        code = part + jnp.where(first, jnp.roll(part, -1, 0), jnp.roll(part, 1, 0))
        acc = jnp.zeros((2 * ROWS, 128), F32)
        for ai in range(7):
            for bi in range(7):
                s = stencil_ref[ai, bi]
                w = jnp.where(code == (ai - 3) * 7 + (bi - 3), s + 1.0, s)
                acc = acc + w * rolled[bi, 2 + 2 * ai : 42 + 2 * ai, pl.ds(l0, 128)]
        adv[ci] = acc
        return carry

    lax.fori_loop(0, NLON // 128, chunk, 0)
    levels = [
        jnp.concatenate([every_other(adv, ci, k) for ci in range(NLON // 128)], axis=1) for k in range(LV)
    ]
    x = jnp.concatenate(
        [v[:, :HALF_LON] + v[:, HALF_LON:] for v in levels] + [v[:, :HALF_LON] - v[:, HALF_LON:] for v in levels], axis=0
    )
    high = x.astype(BF16)
    low = (x - high.astype(F32)).astype(BF16)
    right = jnp.concatenate(
        [
            jnp.concatenate([high, high], axis=1),
            jnp.concatenate([low, jnp.zeros_like(low)], axis=1),
        ],
        axis=0,
    )
    fe[...] = jnp.zeros((N_DEV, 128), F32)
    fo[...] = jnp.zeros((N_DEV, 128), F32)
    fetch.wait()
    for j in range(3):
        prod = lax.dot_general(t_ref[j], right, NT, preferred_element_type=F32)
        fe[:, MSG * j : MSG * (j + 1)] = prod[:, 0:MSG] + prod[:, 2 * MSG : 3 * MSG]
        fo[:, MSG * j : MSG * (j + 1)] = prod[:, MSG : 2 * MSG] + prod[:, 3 * MSG : 4 * MSG]
    out_ref[...] = jnp.where(even_ref[...] > 0.5, fe[...], fo[...])


def every_other(ref, ci, k):
    return ref[ci][k::2] if INTERPRET else ref[ci, pl.ds(k, ROWS, 2), :]


def forward(stencil, tracer, north, south, offsets, table, even):
    return call(
        forward_kernel,
        jax.ShapeDtypeStruct((N_DEV, 128), F32),
        [SM, VM, VM, VM, VM, ANY, VM],
        [
            pltpu.VMEM((64, NLON), F32),
            pltpu.VMEM((7, 64, NLON), F32),
            pltpu.VMEM((2 * ROWS, NLON), jnp.int32),
            pltpu.VMEM((NLON // 128, 2 * ROWS, 128), F32),
            pltpu.VMEM((N_DEV, 128), F32),
            pltpu.VMEM((N_DEV, 128), F32),
            pltpu.VMEM((3, N_DEV, NLON), BF16),
            pltpu.SemaphoreType.DMA,
        ],
        "forward",
        10**9,
    )(stencil, tracer, north, south, offsets, table, even)


def mirror_matrix():
    src = lax.broadcasted_iota(jnp.int32, (128, 128), 0)
    dst = lax.broadcasted_iota(jnp.int32, (128, 128), 1)
    hit = jnp.zeros((128, 128), jnp.bool_)
    for g in range(6):
        hit = jnp.logical_or(
            hit, jnp.logical_and(jnp.logical_and(dst >= 20 * g, dst < 20 * g + 20), src + dst == 40 * g + 19)
        )
    return hit.astype(F32)


def spectral_kernel(
    info_ref,
    msg_ref,
    own_ref,
    shared_ref,
    damping_ref,
    inv_ref,
    vec_ref,
    vecp_ref,
    out_ref,
    spec_ref,
    nbuf,
    sbuf,
    flip,
    zn,
    zs,
    solved,
):
    mirror = mirror_matrix()
    half = N_DEV // 2
    flip[...] = lax.dot_general(msg_ref[half:, :], mirror, NN, precision=HIGH, preferred_element_type=F32)
    for a in range(N_LAT // 2):
        top = msg_ref[16 * a : 16 * a + 16, :]
        low = flip[16 * (15 - a) : 16 * (15 - a) + 16, :]
        for j in range(3):
            for k in range(LV):
                lane = MSG * j + ROWS * k
                nbuf[j, 16 * k : 16 * k + 16, ROWS * a : ROWS * a + ROWS] = top[:, lane : lane + ROWS]
                sbuf[j, 16 * k : 16 * k + 16, ROWS * a : ROWS * a + ROWS] = low[:, lane : lane + ROWS]
    damp = damping_ref[...]

    def exact(left, right):
        return lax.dot_general(left, right, NN, precision=HIGH, preferred_element_type=F32)

    def solve(units, matrix, degree, odd):
        count = len(units)
        hemi = jnp.concatenate(
            [part for j in units for part in (nbuf[j] + sbuf[j], nbuf[j] - sbuf[j])], axis=0
        ).astype(BF16)
        prod = lax.dot_general(hemi, matrix, NT, preferred_element_type=F32)
        keep = degree <= M - 1
        forcing = jnp.concatenate(
            [
                jnp.where(keep, jnp.where(odd, prod[64 * u + 32 : 64 * u + 64], prod[64 * u : 64 * u + 32]), 0.0)
                for u in range(count)
            ],
            axis=0,
        )
        size = 32 * count
        n = degree.astype(F32)
        denominator = 1.0 + (n * (n + 1.0) / float(M * M)) * damp
        modal = exact(inv_ref[:size, :size], forcing)
        modal = jnp.concatenate([modal[32 * u : 32 * u + 32] / denominator for u in range(count)], axis=0)
        packed = exact(vecp_ref[:size, :size], modal)
        left = jnp.concatenate(
            [
                part
                for u in range(count)
                for part in (
                    packed[32 * u : 32 * u + 32],
                    jnp.where(odd, -packed[32 * u : 32 * u + 32], packed[32 * u : 32 * u + 32]),
                )
            ],
            axis=0,
        ).astype(BF16)
        back = lax.dot_general(left, matrix, NN, preferred_element_type=F32)
        for u, j in enumerate(units):
            zn[j] = back[64 * u : 64 * u + 32]
            zs[j] = back[64 * u + 32 : 64 * u + 64]
        return exact(vec_ref[:size, :size], modal).T

    lane = lax.broadcasted_iota(jnp.int32, (32, QP), 1)
    whole = solve((0, 1), own_ref[...], lane + info_ref[0], (lane & 1) == 1)
    lane = lax.broadcasted_iota(jnp.int32, (32, QP // 2), 1)
    block = jnp.floor((lane.astype(F32) + 0.5) * (1.0 / 20.0)).astype(jnp.int32)
    part = solve((2,), shared_ref[...], lane + 20 * block + 20 * info_ref[2] + info_ref[1], (lane & 1) == 1)
    solved[...] = jnp.zeros((N_LEV, QB, 96), F32)
    for b in range(N_LEV):
        solved[b, :, 0:64] = whole[QB * b : QB * b + QB]
        solved[b, 0:20, 64:96] = part[20 * b : 20 * b + 20]
    spec_ref[...] = solved[...].astype(BF16)
    out_ref[...] = jnp.zeros((N_DEV, 128), F32)
    flip[...] = jnp.zeros((half, 128), F32)
    for a in range(N_LAT // 2):
        for j in range(3):
            for k in range(LV):
                lane = MSG * j + ROWS * k
                out_ref[16 * a : 16 * a + 16, lane : lane + ROWS] = zn[j, 16 * k : 16 * k + 16, ROWS * a : ROWS * a + ROWS]
                flip[16 * (15 - a) : 16 * (15 - a) + 16, lane : lane + ROWS] = zs[
                    j, 16 * k : 16 * k + 16, ROWS * a : ROWS * a + ROWS
                ]
    out_ref[half:, :] = lax.dot_general(flip[...], mirror, NN, precision=HIGH, preferred_element_type=F32)


def spectral(info, msgs, own, shared, damping, inv, vec, vecp):
    return call(
        spectral_kernel,
        (jax.ShapeDtypeStruct((N_DEV, 128), F32), jax.ShapeDtypeStruct((N_LEV, QB, 96), BF16)),
        [SM, VM, VM, VM, VM, VM, VM, VM],
        [
            pltpu.VMEM((3, 32, HL), F32),
            pltpu.VMEM((3, 32, HL), F32),
            pltpu.VMEM((N_DEV // 2, 128), F32),
            pltpu.VMEM((3, 32, HL), F32),
            pltpu.VMEM((3, 32, HL), F32),
            pltpu.VMEM((N_LEV, QB, 96), F32),
        ],
        "spectral",
        10**9,
    )(info, msgs, own, shared, damping, inv, vec, vecp)


def inverse_kernel(msg_ref, t_any, even_ref, weight_ref, out_ref, t_ref, t_sem):
    fetch = pltpu.make_async_copy(t_any.at[:, :, pl.ds(0, HALF_LON)], t_ref, t_sem)
    fetch.start()
    lane = lax.broadcasted_iota(jnp.int32, (N_DEV, 128), 1)
    scaled = jnp.where(lane < 3 * MSG, msg_ref[...] * weight_ref[...], 0.0)
    even = (scaled * even_ref[...]).T
    odd = (scaled * (1.0 - even_ref[...])).T
    total = jnp.zeros((2 * MSG, HALF_LON), F32)
    fetch.wait()
    for j in range(3):
        left = jnp.concatenate([even[MSG * j : MSG * (j + 1)], odd[MSG * j : MSG * (j + 1)]], axis=0).astype(BF16)
        total = total + lax.dot_general(left, t_ref[j], NN, preferred_element_type=F32)
    near = total[:MSG] + total[MSG:]
    far = total[:MSG] - total[MSG:]
    for k in range(LV):
        out_ref[:, k, :HALF_LON] = near[ROWS * k : ROWS * (k + 1)]
        out_ref[:, k, HALF_LON:] = far[ROWS * k : ROWS * (k + 1)]


def inverse(msgs, table, even, weight):
    return call(
        inverse_kernel,
        jax.ShapeDtypeStruct((ROWS, LV, NLON), F32),
        [VM, ANY, VM, VM],
        [pltpu.VMEM((3, N_DEV, HALF_LON), BF16), pltpu.SemaphoreType.DMA],
        "inverse",
        10**8,
    )(msgs, table, even, weight)


def place_kernel(spec_ref, out_ref):
    for b in range(N_LEV):
        c, half = (b & 3) >> 1, b & 1
        out_ref[own_slot(b)] = spec_ref[b, :, 0:64].astype(F32)
        out_ref[shared_slot(b), 20 * half : 20 * half + 20, 32 * c : 32 * c + 32] = spec_ref[b, 0:20, 64:96].astype(F32)


def place(spec):
    return call(place_kernel, jax.ShapeDtypeStruct((SLOTS, QB, 64), F32), [VM], [], "place", 10**6)(spec)


def by_block(matrix):
    return jnp.kron(jnp.eye(2, dtype=F32), matrix)


def level_order(value, axis):
    shape = value.shape
    split = shape[:axis] + (16, 2) + shape[axis + 1 :]
    return jnp.swapaxes(value.reshape(split), axis, axis + 1).reshape(shape)


def send_kernel(table_ref, out_ref, sems):
    copies = []
    for b in range(N_LEV):
        copies.append(pltpu.make_async_copy(table_ref.at[own_slot(b)], out_ref.at[b, pl.ds(0, 20)], sems.at[2 * b]))
        half = table_ref.at[shared_slot(b), pl.ds(10 * (b & 1), 10)]
        copies.append(pltpu.make_async_copy(half, out_ref.at[b, pl.ds(20, 10)], sems.at[2 * b + 1]))
    for copy in copies:
        copy.start()
    for copy in copies:
        copy.wait()


def send_tables(legendre):
    return pl.pallas_call(
        send_kernel,
        out_shape=jax.ShapeDtypeStruct((N_LEV, 30, 2, HL), BF16),
        in_specs=[VM],
        out_specs=ANY,
        scratch_shapes=[pltpu.SemaphoreType.DMA((2 * N_LEV,))],
        name="send_tables",
        interpret=INTERPRET,
        cost_estimate=pl.CostEstimate(flops=10**6, bytes_accessed=2 * 10**6, transcendentals=0),
    )(jnp.swapaxes(legendre, 1, 2))


def received_tables(got):
    return got[:, :20].reshape(QP, HL), got[:, 20:].reshape(QP // 2, HL)


def exchange(value, axes):
    return lax.all_to_all(value, axes, split_axis=0, concat_axis=0, tiled=True)


def on_device(tracer, offsets, stencil, assign, legendre, damping, vert_vecs, vert_inv):
    up = [(i, i + 1) for i in range(N_LAT - 1)]
    down = [(i + 1, i) for i in range(N_LAT - 1)]
    rows = jnp.swapaxes(tracer, 0, 1)
    north = lax.ppermute(rows[ROWS - 3 :], "lat", up)
    south = lax.ppermute(rows[:3], "lat", down)
    table, even, weight = tables(assign)
    with jax.named_scope("tabx"):
        matrices = exchange(send_tables(legendre), "lev")
    own, shared = received_tables(matrices)
    msgs = forward(stencil, rows, north, south, jnp.swapaxes(offsets, 0, 1), table, even)
    with jax.named_scope("fwdx"):
        got = exchange(msgs.reshape(N_DEV, 1, 128), ("lat", "lev")).reshape(N_DEV, 128)
    lev = lax.axis_index("lev")
    mine = lax.dynamic_slice_in_dim(assign, lax.axis_index("lat") * SLOTS, SLOTS)
    info = jnp.stack([mine[own_slot(lev)], mine[shared_slot(lev)], lev & 1]).astype(jnp.int32)
    back, spec = spectral(
        info,
        got,
        own,
        shared,
        damping.reshape(32, 1),
        by_block(level_order(vert_inv, 1)),
        by_block(vert_vecs),
        by_block(level_order(vert_vecs, 0)),
    )
    with jax.named_scope("bwdx"):
        home = exchange(back.reshape(N_DEV, 1, 128), ("lat", "lev")).reshape(N_DEV, 128)
    with jax.named_scope("specx"):
        spec = exchange(spec, "lev")
    tracer_new = inverse(home, table, even, weight)
    spectral_new = place(spec).reshape(SLOTS, 20, 2, 64)
    return jnp.swapaxes(tracer_new, 0, 1), jnp.swapaxes(spectral_new, 1, 2)


def solution(mesh):
    placed = (
        P("lev", "lat", None),
        P(None, "lat", None),
        P(),
        P(),
        P("lat", None, "lev", None),
        P(),
        P(),
        P(),
    )
    return jax.shard_map(
        on_device,
        mesh=mesh,
        in_specs=placed,
        out_specs=(P("lev", "lat", None), P("lat", None, "lev", None)),
        check_vma=False,
    )
```

```python
import math

import jax
import jax.numpy as jnp
from jax import lax
from jax.experimental import pallas as pl
from jax.experimental.pallas import tpu as pltpu
from jax.sharding import PartitionSpec as P


INTERPRET = False
N_LAT, N_LEV = 32, 16
N_DEV = N_LAT * N_LEV
M = 640
NLON, HALF_LON = 1280, 640
ROWS = 20
LV = 2
QB = 40
QP = N_LEV * QB
HL = 320
SLOTS = 20
MSG = LV * ROWS
F32, BF16 = jnp.float32, jnp.bfloat16
NT = (((1,), (1,)), ((), ()))
NN = (((1,), (0,)), ((), ()))
HIGH = lax.Precision.HIGHEST


def own_slot(b):
    return 5 * (b >> 2) + (b & 3)


def shared_slot(b):
    return 5 * (b >> 2) + 4


def call(kernel, out_shape, in_specs, scratch, flops=10**7):
    many = isinstance(out_shape, (tuple, list))
    vm = pl.BlockSpec(memory_space=pltpu.VMEM)
    return pl.pallas_call(
        kernel,
        out_shape=out_shape,
        in_specs=in_specs,
        out_specs=[vm] * len(out_shape) if many else vm,
        scratch_shapes=scratch,
        interpret=INTERPRET,
        cost_estimate=pl.CostEstimate(flops=flops, bytes_accessed=10**6, transcendentals=0),
    )


VM = pl.BlockSpec(memory_space=pltpu.VMEM)
ANY = pl.BlockSpec(memory_space=pl.ANY)
SM = pl.BlockSpec(memory_space=pltpu.SMEM)


def cos_sin(phase):
    quad = jnp.floor((phase + 160.5) * (1.0 / 320.0))
    x = (phase - 320.0 * quad) * (2.0 * math.pi / NLON)
    z = x * x
    s = x * (1.0 + z * (-1.6666654611e-1 + z * (8.3321608736e-3 - z * 1.9515295891e-4)))
    c = 1.0 - 0.5 * z + z * z * (
        4.166664568298827e-2 + z * (-1.388731625493765e-3 + z * 2.443315711809948e-5)
    )
    odd = jnp.logical_or(quad == 1.0, quad == 3.0)
    c, s = jnp.where(odd, s, c), jnp.where(odd, c, s)
    c = jnp.where(jnp.logical_or(quad == 1.0, quad == 2.0), -c, c)
    s = jnp.where(jnp.logical_or(quad == 2.0, quad == 3.0), -s, s)
    return c, s


def wrapped(count):
    return count - NLON * jnp.floor((count + 0.5) * (1.0 / NLON))


CHUNK = 64


def tables_kernel(assign_ref, t_ref, even_ref, weight_ref):
    slots = lax.broadcasted_iota(jnp.int32, (CHUNK, M), 1)
    lane = lax.broadcasted_iota(jnp.int32, (CHUNK, 128), 1)
    lane_f = lane.astype(F32)
    assign = assign_ref[...].reshape(1, M).astype(F32)

    def step(i, carry):
        r0 = pl.multiple_of(i * CHUNK, CHUNK)
        d = r0 + lax.broadcasted_iota(jnp.int32, (CHUNK, 1), 0)
        lev = d & 15
        waves, evens, weights = [], [], []
        for slot in (own_slot(lev), shared_slot(lev)):
            wave = jnp.sum(jnp.where(slots == (d >> 4) * SLOTS + slot, assign, 0.0), axis=1, keepdims=True)
            waves.append(wave)
            evens.append(jnp.where(wave == 2.0 * jnp.floor(wave * 0.5), 1.0, 0.0))
            weights.append(jnp.where(wave == 0.0, 1.0, 2.0))
        turn_c, turn_s = cos_sin(wrapped(jnp.where(lane == 0, waves[0], waves[1]) * 128.0))

        def put(j, block, value):
            high = value.astype(BF16)
            t_ref[j, pl.ds(r0, CHUNK), 128 * block : 128 * block + 128] = high
            low = (value - high.astype(F32)).astype(BF16)
            t_ref[j, pl.ds(r0, CHUNK), HALF_LON + 128 * block : HALF_LON + 128 * block + 128] = low

        for u in range(2):
            start = wrapped(waves[u] * lane_f + (jnp.where((lev & 2) == 2, 320.0, 0.0) if u else 0.0))
            c, s = cos_sin(start)
            c = c * (1.0 / math.sqrt(NLON))
            s = s * (1.0 / math.sqrt(NLON))
            cd, sd = turn_c[:, u : u + 1], turn_s[:, u : u + 1]
            for block in range(5):
                put(2 * u, block, c)
                if u == 0:
                    put(1, block, -s)
                if block < 4:
                    c, s = c * cd - s * sd, s * cd + c * sd
        even_ref[pl.ds(r0, CHUNK), :] = jnp.where(
            lane < 2 * MSG, evens[0], evens[1]
        )
        weight_ref[pl.ds(r0, CHUNK), :] = jnp.where(
            lane < 2 * MSG, weights[0], weights[1]
        )
        return carry

    lax.fori_loop(0, N_DEV // CHUNK, step, 0)


def tables(assign):
    return call(
        tables_kernel,
        (
            jax.ShapeDtypeStruct((3, N_DEV, NLON), BF16),
            jax.ShapeDtypeStruct((N_DEV, 128), F32),
            jax.ShapeDtypeStruct((N_DEV, 128), F32),
        ),
        [VM],
        [],
    )(assign)


def forward_kernel(
    stencil_ref,
    tracer_ref,
    north_ref,
    south_ref,
    off_ref,
    t_any,
    even_ref,
    out_ref,
    pad,
    rolled,
    codes,
    adv,
    fe,
    fo,
    t_ref,
    t_sem,
):
    fetch = pltpu.make_async_copy(t_any, t_ref, t_sem)
    fetch.start()
    pad[...] = jnp.zeros((64, NLON), F32)
    for i in range(3):
        pad[2 + 2 * i : 4 + 2 * i, :] = north_ref[i]
        pad[48 + 2 * i : 50 + 2 * i, :] = south_ref[i]
    for i in range(ROWS):
        pad[8 + 2 * i : 10 + 2 * i, :] = tracer_ref[i]
        codes[2 * i : 2 * i + 2, :] = off_ref[i]
    for bi in range(7):
        shift = (3 - bi) % NLON
        rolled[bi] = pltpu.roll(pad[...], shift, 1) if shift else pad[...]

    first = (lax.broadcasted_iota(jnp.int32, (2 * ROWS, 128), 0) & 1) == 0

    def chunk(ci, carry):
        l0 = pl.multiple_of(ci * 128, 128)
        value = codes[:, pl.ds(l0, 128)]
        part = jnp.where(first, value * 7, value)
        code = part + jnp.where(first, jnp.roll(part, -1, 0), jnp.roll(part, 1, 0))
        acc = jnp.zeros((2 * ROWS, 128), F32)
        for ai in range(7):
            for bi in range(7):
                s = stencil_ref[ai, bi]
                w = jnp.where(code == (ai - 3) * 7 + (bi - 3), s + 1.0, s)
                acc = acc + w * rolled[bi, 2 + 2 * ai : 42 + 2 * ai, pl.ds(l0, 128)]
        adv[ci] = acc
        return carry

    lax.fori_loop(0, NLON // 128, chunk, 0)
    levels = [
        jnp.concatenate([every_other(adv, ci, k) for ci in range(NLON // 128)], axis=1) for k in range(LV)
    ]
    x = jnp.concatenate(
        [v[:, :HALF_LON] + v[:, HALF_LON:] for v in levels] + [v[:, :HALF_LON] - v[:, HALF_LON:] for v in levels], axis=0
    )
    high = x.astype(BF16)
    low = (x - high.astype(F32)).astype(BF16)
    right = jnp.concatenate(
        [
            jnp.concatenate([high, high], axis=1),
            jnp.concatenate([low, jnp.zeros_like(low)], axis=1),
        ],
        axis=0,
    )
    fe[...] = jnp.zeros((N_DEV, 128), F32)
    fo[...] = jnp.zeros((N_DEV, 128), F32)
    fetch.wait()
    for j in range(3):
        prod = lax.dot_general(t_ref[j], right, NT, preferred_element_type=F32)
        fe[:, MSG * j : MSG * (j + 1)] = prod[:, 0:MSG] + prod[:, 2 * MSG : 3 * MSG]
        fo[:, MSG * j : MSG * (j + 1)] = prod[:, MSG : 2 * MSG] + prod[:, 3 * MSG : 4 * MSG]
    out_ref[...] = jnp.where(even_ref[...] > 0.5, fe[...], fo[...])


def every_other(ref, ci, k):
    return ref[ci][k::2] if INTERPRET else ref[ci, pl.ds(k, ROWS, 2), :]


def forward(stencil, tracer, north, south, offsets, table, even):
    return call(
        forward_kernel,
        jax.ShapeDtypeStruct((N_DEV, 128), F32),
        [SM, VM, VM, VM, VM, ANY, VM],
        [
            pltpu.VMEM((64, NLON), F32),
            pltpu.VMEM((7, 64, NLON), F32),
            pltpu.VMEM((2 * ROWS, NLON), jnp.int32),
            pltpu.VMEM((NLON // 128, 2 * ROWS, 128), F32),
            pltpu.VMEM((N_DEV, 128), F32),
            pltpu.VMEM((N_DEV, 128), F32),
            pltpu.VMEM((3, N_DEV, NLON), BF16),
            pltpu.SemaphoreType.DMA,
        ],
        10**9,
    )(stencil, tracer, north, south, offsets, table, even)


def mirror_matrix():
    src = lax.broadcasted_iota(jnp.int32, (128, 128), 0)
    dst = lax.broadcasted_iota(jnp.int32, (128, 128), 1)
    hit = jnp.zeros((128, 128), jnp.bool_)
    for g in range(6):
        hit = jnp.logical_or(
            hit, jnp.logical_and(jnp.logical_and(dst >= 20 * g, dst < 20 * g + 20), src + dst == 40 * g + 19)
        )
    return hit.astype(F32)


def spectral_kernel(
    info_ref,
    msg_ref,
    own_ref,
    shared_ref,
    damping_ref,
    inv_ref,
    vec_ref,
    vecp_ref,
    out_ref,
    spec_ref,
    nbuf,
    sbuf,
    flip,
    zn,
    zs,
    solved,
):
    mirror = mirror_matrix()
    half = N_DEV // 2
    flip[...] = lax.dot_general(msg_ref[half:, :], mirror, NN, precision=HIGH, preferred_element_type=F32)
    for a in range(N_LAT // 2):
        top = msg_ref[16 * a : 16 * a + 16, :]
        low = flip[16 * (15 - a) : 16 * (15 - a) + 16, :]
        for j in range(3):
            for k in range(LV):
                lane = MSG * j + ROWS * k
                nbuf[j, 16 * k : 16 * k + 16, ROWS * a : ROWS * a + ROWS] = top[:, lane : lane + ROWS]
                sbuf[j, 16 * k : 16 * k + 16, ROWS * a : ROWS * a + ROWS] = low[:, lane : lane + ROWS]
    damp = damping_ref[...]

    def exact(left, right):
        return lax.dot_general(left, right, NN, precision=HIGH, preferred_element_type=F32)

    def solve(units, matrix, degree, odd):
        count = len(units)
        hemi = jnp.concatenate(
            [part for j in units for part in (nbuf[j] + sbuf[j], nbuf[j] - sbuf[j])], axis=0
        ).astype(BF16)
        prod = lax.dot_general(hemi, matrix, NT, preferred_element_type=F32)
        keep = degree <= M - 1
        forcing = jnp.concatenate(
            [
                jnp.where(keep, jnp.where(odd, prod[64 * u + 32 : 64 * u + 64], prod[64 * u : 64 * u + 32]), 0.0)
                for u in range(count)
            ],
            axis=0,
        )
        size = 32 * count
        n = degree.astype(F32)
        denominator = 1.0 + (n * (n + 1.0) / float(M * M)) * damp
        modal = exact(inv_ref[:size, :size], forcing)
        modal = jnp.concatenate([modal[32 * u : 32 * u + 32] / denominator for u in range(count)], axis=0)
        packed = exact(vecp_ref[:size, :size], modal)
        left = jnp.concatenate(
            [
                part
                for u in range(count)
                for part in (
                    packed[32 * u : 32 * u + 32],
                    jnp.where(odd, -packed[32 * u : 32 * u + 32], packed[32 * u : 32 * u + 32]),
                )
            ],
            axis=0,
        ).astype(BF16)
        back = lax.dot_general(left, matrix, NN, preferred_element_type=F32)
        for u, j in enumerate(units):
            zn[j] = back[64 * u : 64 * u + 32]
            zs[j] = back[64 * u + 32 : 64 * u + 64]
        return exact(vec_ref[:size, :size], modal).T

    lane = lax.broadcasted_iota(jnp.int32, (32, QP), 1)
    whole = solve((0, 1), own_ref[...], lane + info_ref[0], (lane & 1) == 1)
    lane = lax.broadcasted_iota(jnp.int32, (32, QP // 2), 1)
    block = jnp.floor((lane.astype(F32) + 0.5) * (1.0 / 20.0)).astype(jnp.int32)
    part = solve((2,), shared_ref[...], lane + 20 * block + 20 * info_ref[2] + info_ref[1], (lane & 1) == 1)
    solved[...] = jnp.zeros((N_LEV, QB, 96), F32)
    for b in range(N_LEV):
        solved[b, :, 0:64] = whole[QB * b : QB * b + QB]
        solved[b, 0:20, 64:96] = part[20 * b : 20 * b + 20]
    spec_ref[...] = solved[...].astype(BF16)
    out_ref[...] = jnp.zeros((N_DEV, 128), F32)
    flip[...] = jnp.zeros((half, 128), F32)
    for a in range(N_LAT // 2):
        for j in range(3):
            for k in range(LV):
                lane = MSG * j + ROWS * k
                out_ref[16 * a : 16 * a + 16, lane : lane + ROWS] = zn[j, 16 * k : 16 * k + 16, ROWS * a : ROWS * a + ROWS]
                flip[16 * (15 - a) : 16 * (15 - a) + 16, lane : lane + ROWS] = zs[
                    j, 16 * k : 16 * k + 16, ROWS * a : ROWS * a + ROWS
                ]
    out_ref[half:, :] = lax.dot_general(flip[...], mirror, NN, precision=HIGH, preferred_element_type=F32)


def spectral(info, msgs, own, shared, damping, inv, vec, vecp):
    return call(
        spectral_kernel,
        (jax.ShapeDtypeStruct((N_DEV, 128), F32), jax.ShapeDtypeStruct((N_LEV, QB, 96), BF16)),
        [SM, VM, VM, VM, VM, VM, VM, VM],
        [
            pltpu.VMEM((3, 32, HL), F32),
            pltpu.VMEM((3, 32, HL), F32),
            pltpu.VMEM((N_DEV // 2, 128), F32),
            pltpu.VMEM((3, 32, HL), F32),
            pltpu.VMEM((3, 32, HL), F32),
            pltpu.VMEM((N_LEV, QB, 96), F32),
        ],
        10**9,
    )(info, msgs, own, shared, damping, inv, vec, vecp)


def inverse_kernel(msg_ref, t_any, even_ref, weight_ref, out_ref, t_ref, t_sem):
    fetch = pltpu.make_async_copy(t_any.at[:, :, pl.ds(0, HALF_LON)], t_ref, t_sem)
    fetch.start()
    lane = lax.broadcasted_iota(jnp.int32, (N_DEV, 128), 1)
    scaled = jnp.where(lane < 3 * MSG, msg_ref[...] * weight_ref[...], 0.0)
    even = (scaled * even_ref[...]).T
    odd = (scaled * (1.0 - even_ref[...])).T
    total = jnp.zeros((2 * MSG, HALF_LON), F32)
    fetch.wait()
    for j in range(3):
        left = jnp.concatenate([even[MSG * j : MSG * (j + 1)], odd[MSG * j : MSG * (j + 1)]], axis=0).astype(BF16)
        total = total + lax.dot_general(left, t_ref[j], NN, preferred_element_type=F32)
    near = total[:MSG] + total[MSG:]
    far = total[:MSG] - total[MSG:]
    for k in range(LV):
        out_ref[:, k, :HALF_LON] = near[ROWS * k : ROWS * (k + 1)]
        out_ref[:, k, HALF_LON:] = far[ROWS * k : ROWS * (k + 1)]


def inverse(msgs, table, even, weight):
    return call(
        inverse_kernel,
        jax.ShapeDtypeStruct((ROWS, LV, NLON), F32),
        [VM, ANY, VM, VM],
        [pltpu.VMEM((3, N_DEV, HALF_LON), BF16), pltpu.SemaphoreType.DMA],
        10**8,
    )(msgs, table, even, weight)


def place_kernel(spec_ref, out_ref):
    for b in range(N_LEV):
        c, half = (b & 3) >> 1, b & 1
        out_ref[own_slot(b)] = spec_ref[b, :, 0:64].astype(F32)
        out_ref[shared_slot(b), 20 * half : 20 * half + 20, 32 * c : 32 * c + 32] = spec_ref[b, 0:20, 64:96].astype(F32)


def place(spec):
    return call(place_kernel, jax.ShapeDtypeStruct((SLOTS, QB, 64), F32), [VM], [], 10**6)(spec)


def by_block(matrix):
    return jnp.kron(jnp.eye(2, dtype=F32), matrix)


def level_order(value, axis):
    shape = value.shape
    split = shape[:axis] + (16, 2) + shape[axis + 1 :]
    return jnp.swapaxes(value.reshape(split), axis, axis + 1).reshape(shape)


def send_kernel(table_ref, out_ref, sems):
    copies = []
    for b in range(N_LEV):
        copies.append(pltpu.make_async_copy(table_ref.at[own_slot(b)], out_ref.at[b, pl.ds(0, 20)], sems.at[2 * b]))
        half = table_ref.at[shared_slot(b), pl.ds(10 * (b & 1), 10)]
        copies.append(pltpu.make_async_copy(half, out_ref.at[b, pl.ds(20, 10)], sems.at[2 * b + 1]))
    for copy in copies:
        copy.start()
    for copy in copies:
        copy.wait()


def send_tables(legendre):
    return pl.pallas_call(
        send_kernel,
        out_shape=jax.ShapeDtypeStruct((N_LEV, 30, 2, HL), BF16),
        in_specs=[VM],
        out_specs=ANY,
        scratch_shapes=[pltpu.SemaphoreType.DMA((2 * N_LEV,))],
        name="send_tables",
        interpret=INTERPRET,
        cost_estimate=pl.CostEstimate(flops=10**6, bytes_accessed=2 * 10**6, transcendentals=0),
    )(jnp.swapaxes(legendre, 1, 2))


def received_tables(got):
    return got[:, :20].reshape(QP, HL), got[:, 20:].reshape(QP // 2, HL)


def exchange(value, axes):
    return lax.all_to_all(value, axes, split_axis=0, concat_axis=0, tiled=True)


def step_of(tracer, offsets, stencil, assign, legendre, damping, vert_vecs, vert_inv):
    up = [(i, i + 1) for i in range(N_LAT - 1)]
    down = [(i + 1, i) for i in range(N_LAT - 1)]
    rows = jnp.swapaxes(tracer, 0, 1)
    north = lax.ppermute(rows[ROWS - 3 :], "lat", up)
    south = lax.ppermute(rows[:3], "lat", down)
    table, even, weight = tables(assign)
    packed = send_tables(legendre)
    matrices = exchange(packed, "lev")
    own, shared = received_tables(matrices)
    msgs = forward(stencil, rows, north, south, jnp.swapaxes(offsets, 0, 1), table, even)
    got = exchange(msgs.reshape(N_DEV, 1, 128), ("lat", "lev")).reshape(N_DEV, 128)
    lev = lax.axis_index("lev")
    mine = lax.dynamic_slice_in_dim(assign, lax.axis_index("lat") * SLOTS, SLOTS)
    info = jnp.stack([mine[own_slot(lev)], mine[shared_slot(lev)], lev & 1]).astype(jnp.int32)
    back, spec = spectral(
        info,
        got,
        own,
        shared,
        damping.reshape(32, 1),
        by_block(level_order(vert_inv, 1)),
        by_block(vert_vecs),
        by_block(level_order(vert_vecs, 0)),
    )
    home = exchange(back.reshape(N_DEV, 1, 128), ("lat", "lev")).reshape(N_DEV, 128)
    spec = exchange(spec, "lev")
    tracer_new = inverse(home, table, even, weight)
    spectral_new = place(spec).reshape(SLOTS, 20, 2, 64)
    return jnp.swapaxes(tracer_new, 0, 1), jnp.swapaxes(spectral_new, 1, 2)


def solution(mesh):
    placed = (
        P("lev", "lat", None),
        P(None, "lat", None),
        P(),
        P(),
        P("lat", None, "lev", None),
        P(),
        P(),
        P(),
    )
    return jax.shard_map(
        step_of,
        mesh=mesh,
        in_specs=placed,
        out_specs=(P("lev", "lat", None), P("lat", None, "lev", None)),
        check_vma=False,
    )
```

```python
import math

import jax
import jax.numpy as jnp
from jax import lax
from jax.experimental import pallas as pl
from jax.experimental.pallas import tpu as pltpu
from jax.sharding import PartitionSpec as P


INTERPRET = False
N_LAT, N_LEV = 32, 16
N_DEV = N_LAT * N_LEV
M = 640
NLON, HALF_LON = 1280, 640
ROWS = 20
LV = 2
QB = 40
QP = N_LEV * QB
HL = 320
SLOTS = 20
MSG = LV * ROWS
F32, BF16 = jnp.float32, jnp.bfloat16
NT = (((1,), (1,)), ((), ()))
NN = (((1,), (0,)), ((), ()))
HIGH = lax.Precision.HIGHEST


def own_slot(b):
    return 5 * (b >> 2) + (b & 3)


def shared_slot(b):
    return 5 * (b >> 2) + 4


def call(kernel, out_shape, in_specs, scratch, flops=10**7):
    many = isinstance(out_shape, (tuple, list))
    vm = pl.BlockSpec(memory_space=pltpu.VMEM)
    return pl.pallas_call(
        kernel,
        out_shape=out_shape,
        in_specs=in_specs,
        out_specs=[vm] * len(out_shape) if many else vm,
        scratch_shapes=scratch,
        interpret=INTERPRET,
        cost_estimate=pl.CostEstimate(flops=flops, bytes_accessed=10**6, transcendentals=0),
    )


VM = pl.BlockSpec(memory_space=pltpu.VMEM)
ANY = pl.BlockSpec(memory_space=pl.ANY)
SM = pl.BlockSpec(memory_space=pltpu.SMEM)


def cos_sin(phase):
    quad = jnp.floor((phase + 160.5) * (1.0 / 320.0))
    x = (phase - 320.0 * quad) * (2.0 * math.pi / NLON)
    z = x * x
    s = x * (1.0 + z * (-1.6666654611e-1 + z * (8.3321608736e-3 - z * 1.9515295891e-4)))
    c = 1.0 - 0.5 * z + z * z * (
        4.166664568298827e-2 + z * (-1.388731625493765e-3 + z * 2.443315711809948e-5)
    )
    odd = jnp.logical_or(quad == 1.0, quad == 3.0)
    c, s = jnp.where(odd, s, c), jnp.where(odd, c, s)
    c = jnp.where(jnp.logical_or(quad == 1.0, quad == 2.0), -c, c)
    s = jnp.where(jnp.logical_or(quad == 2.0, quad == 3.0), -s, s)
    return c, s


def wrapped(count):
    return count - NLON * jnp.floor((count + 0.5) * (1.0 / NLON))


CHUNK = 64


def tables_kernel(assign_ref, t_out, even_ref, weight_ref, t_ref, sems):
    def write(i):
        rows = pl.ds(pl.multiple_of(i * CHUNK, CHUNK), CHUNK)
        return pltpu.make_async_copy(t_ref.at[:, rows], t_out.at[:, rows], sems.at[i])

    slots = lax.broadcasted_iota(jnp.int32, (CHUNK, M), 1)
    lane = lax.broadcasted_iota(jnp.int32, (CHUNK, 128), 1)
    lane_f = lane.astype(F32)
    assign = assign_ref[...].reshape(1, M).astype(F32)

    def step(i, carry):
        r0 = pl.multiple_of(i * CHUNK, CHUNK)
        d = r0 + lax.broadcasted_iota(jnp.int32, (CHUNK, 1), 0)
        lev = d & 15
        waves, evens, weights = [], [], []
        for slot in (own_slot(lev), shared_slot(lev)):
            wave = jnp.sum(jnp.where(slots == (d >> 4) * SLOTS + slot, assign, 0.0), axis=1, keepdims=True)
            waves.append(wave)
            evens.append(jnp.where(wave == 2.0 * jnp.floor(wave * 0.5), 1.0, 0.0))
            weights.append(jnp.where(wave == 0.0, 1.0, 2.0))
        turn_c, turn_s = cos_sin(wrapped(jnp.where(lane == 0, waves[0], waves[1]) * 128.0))

        def put(j, block, value):
            high = value.astype(BF16)
            t_ref[j, pl.ds(r0, CHUNK), 128 * block : 128 * block + 128] = high
            low = (value - high.astype(F32)).astype(BF16)
            t_ref[j, pl.ds(r0, CHUNK), HALF_LON + 128 * block : HALF_LON + 128 * block + 128] = low

        for u in range(2):
            start = wrapped(waves[u] * lane_f + (jnp.where((lev & 2) == 2, 320.0, 0.0) if u else 0.0))
            c, s = cos_sin(start)
            c = c * (1.0 / math.sqrt(NLON))
            s = s * (1.0 / math.sqrt(NLON))
            cd, sd = turn_c[:, u : u + 1], turn_s[:, u : u + 1]
            for block in range(5):
                put(2 * u, block, c)
                if u == 0:
                    put(1, block, -s)
                if block < 4:
                    c, s = c * cd - s * sd, s * cd + c * sd
        even_ref[pl.ds(r0, CHUNK), :] = jnp.where(
            lane < 2 * MSG, evens[0], evens[1]
        )
        weight_ref[pl.ds(r0, CHUNK), :] = jnp.where(
            lane < 2 * MSG, weights[0], weights[1]
        )
        write(i).start()
        return carry

    lax.fori_loop(0, N_DEV // CHUNK, step, 0)
    for i in range(N_DEV // CHUNK):
        write(i).wait()


def tables(assign):
    return pl.pallas_call(
        tables_kernel,
        out_shape=(
            jax.ShapeDtypeStruct((3, N_DEV, NLON), BF16),
            jax.ShapeDtypeStruct((N_DEV, 128), F32),
            jax.ShapeDtypeStruct((N_DEV, 128), F32),
        ),
        in_specs=[VM],
        out_specs=(ANY, VM, VM),
        scratch_shapes=[pltpu.VMEM((3, N_DEV, NLON), BF16), pltpu.SemaphoreType.DMA((N_DEV // CHUNK,))],
        name="tables",
        interpret=INTERPRET,
        cost_estimate=pl.CostEstimate(flops=10**7, bytes_accessed=10**6, transcendentals=0),
    )(assign)


def forward_kernel(
    side_ref,
    stencil_ref,
    tracer_ref,
    near_ref,
    far_ref,
    off_ref,
    t_any,
    even_ref,
    out_ref,
    pad,
    rolled,
    codes,
    adv,
    fe,
    fo,
    t_ref,
    t_sem,
):
    fetch = pltpu.make_async_copy(t_any, t_ref, t_sem)
    fetch.start()
    odd_band = side_ref[0] == 1
    pad[...] = jnp.zeros((64, NLON), F32)
    for i in range(3):
        pad[2 + 2 * i : 4 + 2 * i, :] = jnp.where(odd_band, near_ref[i], far_ref[i])
        pad[48 + 2 * i : 50 + 2 * i, :] = jnp.where(odd_band, far_ref[i], near_ref[i])
    for i in range(ROWS):
        pad[8 + 2 * i : 10 + 2 * i, :] = tracer_ref[i]
        codes[2 * i : 2 * i + 2, :] = off_ref[i]
    for bi in range(7):
        shift = (3 - bi) % NLON
        rolled[bi] = pltpu.roll(pad[...], shift, 1) if shift else pad[...]

    first = (lax.broadcasted_iota(jnp.int32, (2 * ROWS, 128), 0) & 1) == 0

    def chunk(ci, carry):
        l0 = pl.multiple_of(ci * 128, 128)
        value = codes[:, pl.ds(l0, 128)]
        part = jnp.where(first, value * 7, value)
        code = part + jnp.where(first, jnp.roll(part, -1, 0), jnp.roll(part, 1, 0))
        acc = jnp.zeros((2 * ROWS, 128), F32)
        for ai in range(7):
            for bi in range(7):
                s = stencil_ref[ai, bi]
                w = jnp.where(code == (ai - 3) * 7 + (bi - 3), s + 1.0, s)
                acc = acc + w * rolled[bi, 2 + 2 * ai : 42 + 2 * ai, pl.ds(l0, 128)]
        adv[ci] = acc
        return carry

    lax.fori_loop(0, NLON // 128, chunk, 0)
    levels = [
        jnp.concatenate([every_other(adv, ci, k) for ci in range(NLON // 128)], axis=1) for k in range(LV)
    ]
    x = jnp.concatenate(
        [v[:, :HALF_LON] + v[:, HALF_LON:] for v in levels] + [v[:, :HALF_LON] - v[:, HALF_LON:] for v in levels], axis=0
    )
    high = x.astype(BF16)
    low = (x - high.astype(F32)).astype(BF16)
    right = jnp.concatenate(
        [
            jnp.concatenate([high, high], axis=1),
            jnp.concatenate([low, jnp.zeros_like(low)], axis=1),
        ],
        axis=0,
    )
    fe[...] = jnp.zeros((N_DEV, 128), F32)
    fo[...] = jnp.zeros((N_DEV, 128), F32)
    fetch.wait()
    for j in range(3):
        prod = lax.dot_general(t_ref[j], right, NT, preferred_element_type=F32)
        fe[:, MSG * j : MSG * (j + 1)] = prod[:, 0:MSG] + prod[:, 2 * MSG : 3 * MSG]
        fo[:, MSG * j : MSG * (j + 1)] = prod[:, MSG : 2 * MSG] + prod[:, 3 * MSG : 4 * MSG]
    out_ref[...] = jnp.where(even_ref[...] > 0.5, fe[...], fo[...])


def every_other(ref, ci, k):
    return ref[ci][k::2] if INTERPRET else ref[ci, pl.ds(k, ROWS, 2), :]


def forward(side, stencil, tracer, near, far, offsets, table, even):
    return call(
        forward_kernel,
        jax.ShapeDtypeStruct((N_DEV, 128), F32),
        [SM, SM, VM, VM, VM, VM, ANY, VM],
        [
            pltpu.VMEM((64, NLON), F32),
            pltpu.VMEM((7, 64, NLON), F32),
            pltpu.VMEM((2 * ROWS, NLON), jnp.int32),
            pltpu.VMEM((NLON // 128, 2 * ROWS, 128), F32),
            pltpu.VMEM((N_DEV, 128), F32),
            pltpu.VMEM((N_DEV, 128), F32),
            pltpu.VMEM((3, N_DEV, NLON), BF16),
            pltpu.SemaphoreType.DMA,
        ],
        10**9,
    )(side, stencil, tracer, near, far, offsets, table, even)


def mirror_matrix():
    src = lax.broadcasted_iota(jnp.int32, (128, 128), 0)
    dst = lax.broadcasted_iota(jnp.int32, (128, 128), 1)
    hit = jnp.zeros((128, 128), jnp.bool_)
    for g in range(6):
        hit = jnp.logical_or(
            hit, jnp.logical_and(jnp.logical_and(dst >= 20 * g, dst < 20 * g + 20), src + dst == 40 * g + 19)
        )
    return hit.astype(F32)


def spectral_kernel(
    info_ref,
    msg_ref,
    own_ref,
    shared_ref,
    damping_ref,
    inv_ref,
    vec_ref,
    vecp_ref,
    out_ref,
    spec_ref,
    nbuf,
    sbuf,
    flip,
    zn,
    zs,
    solved,
):
    mirror = mirror_matrix()
    half = N_DEV // 2
    flip[...] = lax.dot_general(msg_ref[half:, :], mirror, NN, precision=HIGH, preferred_element_type=F32)
    for a in range(N_LAT // 2):
        top = msg_ref[16 * a : 16 * a + 16, :]
        low = flip[16 * (15 - a) : 16 * (15 - a) + 16, :]
        for j in range(3):
            for k in range(LV):
                lane = MSG * j + ROWS * k
                nbuf[j, 16 * k : 16 * k + 16, ROWS * a : ROWS * a + ROWS] = top[:, lane : lane + ROWS]
                sbuf[j, 16 * k : 16 * k + 16, ROWS * a : ROWS * a + ROWS] = low[:, lane : lane + ROWS]
    damp = damping_ref[...]

    def exact(left, right):
        return lax.dot_general(left, right, NN, precision=HIGH, preferred_element_type=F32)

    def solve(units, matrix, degree, odd):
        count = len(units)
        hemi = jnp.concatenate(
            [part for j in units for part in (nbuf[j] + sbuf[j], nbuf[j] - sbuf[j])], axis=0
        ).astype(BF16)
        prod = lax.dot_general(hemi, matrix, NT, preferred_element_type=F32)
        keep = degree <= M - 1
        forcing = jnp.concatenate(
            [
                jnp.where(keep, jnp.where(odd, prod[64 * u + 32 : 64 * u + 64], prod[64 * u : 64 * u + 32]), 0.0)
                for u in range(count)
            ],
            axis=0,
        )
        size = 32 * count
        n = degree.astype(F32)
        denominator = 1.0 + (n * (n + 1.0) / float(M * M)) * damp
        modal = exact(inv_ref[:size, :size], forcing)
        modal = jnp.concatenate([modal[32 * u : 32 * u + 32] / denominator for u in range(count)], axis=0)
        packed = exact(vecp_ref[:size, :size], modal)
        left = jnp.concatenate(
            [
                part
                for u in range(count)
                for part in (
                    packed[32 * u : 32 * u + 32],
                    jnp.where(odd, -packed[32 * u : 32 * u + 32], packed[32 * u : 32 * u + 32]),
                )
            ],
            axis=0,
        ).astype(BF16)
        back = lax.dot_general(left, matrix, NN, preferred_element_type=F32)
        for u, j in enumerate(units):
            zn[j] = back[64 * u : 64 * u + 32]
            zs[j] = back[64 * u + 32 : 64 * u + 64]
        return exact(vec_ref[:size, :size], modal).T

    lane = lax.broadcasted_iota(jnp.int32, (32, QP), 1)
    whole = solve((0, 1), own_ref[...], lane + info_ref[0], (lane & 1) == 1)
    lane = lax.broadcasted_iota(jnp.int32, (32, QP // 2), 1)
    block = jnp.floor((lane.astype(F32) + 0.5) * (1.0 / 20.0)).astype(jnp.int32)
    part = solve((2,), shared_ref[...], lane + 20 * block + 20 * info_ref[2] + info_ref[1], (lane & 1) == 1)
    solved[...] = jnp.zeros((N_LEV, QB, 96), F32)
    for b in range(N_LEV):
        solved[b, :, 0:64] = whole[QB * b : QB * b + QB]
        solved[b, 0:20, 64:96] = part[20 * b : 20 * b + 20]
    spec_ref[...] = solved[...].astype(BF16)
    out_ref[...] = jnp.zeros((N_DEV, 128), F32)
    flip[...] = jnp.zeros((half, 128), F32)
    for a in range(N_LAT // 2):
        for j in range(3):
            for k in range(LV):
                lane = MSG * j + ROWS * k
                out_ref[16 * a : 16 * a + 16, lane : lane + ROWS] = zn[j, 16 * k : 16 * k + 16, ROWS * a : ROWS * a + ROWS]
                flip[16 * (15 - a) : 16 * (15 - a) + 16, lane : lane + ROWS] = zs[
                    j, 16 * k : 16 * k + 16, ROWS * a : ROWS * a + ROWS
                ]
    out_ref[half:, :] = lax.dot_general(flip[...], mirror, NN, precision=HIGH, preferred_element_type=F32)


def spectral(info, msgs, own, shared, damping, inv, vec, vecp):
    return call(
        spectral_kernel,
        (jax.ShapeDtypeStruct((N_DEV, 128), F32), jax.ShapeDtypeStruct((N_LEV, QB, 96), BF16)),
        [SM, VM, VM, VM, VM, VM, VM, VM],
        [
            pltpu.VMEM((3, 32, HL), F32),
            pltpu.VMEM((3, 32, HL), F32),
            pltpu.VMEM((N_DEV // 2, 128), F32),
            pltpu.VMEM((3, 32, HL), F32),
            pltpu.VMEM((3, 32, HL), F32),
            pltpu.VMEM((N_LEV, QB, 96), F32),
        ],
        10**9,
    )(info, msgs, own, shared, damping, inv, vec, vecp)


def inverse_kernel(msg_ref, t_any, even_ref, weight_ref, out_ref, t_ref, t_sem):
    fetch = pltpu.make_async_copy(t_any.at[:, :, pl.ds(0, HALF_LON)], t_ref, t_sem)
    fetch.start()
    lane = lax.broadcasted_iota(jnp.int32, (N_DEV, 128), 1)
    scaled = jnp.where(lane < 3 * MSG, msg_ref[...] * weight_ref[...], 0.0)
    even = (scaled * even_ref[...]).T
    odd = (scaled * (1.0 - even_ref[...])).T
    total = jnp.zeros((2 * MSG, HALF_LON), F32)
    fetch.wait()
    for j in range(3):
        left = jnp.concatenate([even[MSG * j : MSG * (j + 1)], odd[MSG * j : MSG * (j + 1)]], axis=0).astype(BF16)
        total = total + lax.dot_general(left, t_ref[j], NN, preferred_element_type=F32)
    near = total[:MSG] + total[MSG:]
    far = total[:MSG] - total[MSG:]
    for k in range(LV):
        out_ref[:, k, :HALF_LON] = near[ROWS * k : ROWS * (k + 1)]
        out_ref[:, k, HALF_LON:] = far[ROWS * k : ROWS * (k + 1)]


def inverse(msgs, table, even, weight):
    return call(
        inverse_kernel,
        jax.ShapeDtypeStruct((ROWS, LV, NLON), F32),
        [VM, ANY, VM, VM],
        [pltpu.VMEM((3, N_DEV, HALF_LON), BF16), pltpu.SemaphoreType.DMA],
        10**8,
    )(msgs, table, even, weight)


def place_kernel(spec_ref, out_ref):
    for b in range(N_LEV):
        c, half = (b & 3) >> 1, b & 1
        out_ref[own_slot(b)] = spec_ref[b, :, 0:64].astype(F32)
        out_ref[shared_slot(b), 20 * half : 20 * half + 20, 32 * c : 32 * c + 32] = spec_ref[b, 0:20, 64:96].astype(F32)


def place(spec):
    return call(place_kernel, jax.ShapeDtypeStruct((SLOTS, QB, 64), F32), [VM], [], 10**6)(spec)


def by_block(matrix):
    return jnp.kron(jnp.eye(2, dtype=F32), matrix)


def level_order(value, axis):
    shape = value.shape
    split = shape[:axis] + (16, 2) + shape[axis + 1 :]
    return jnp.swapaxes(value.reshape(split), axis, axis + 1).reshape(shape)


def send_kernel(table_ref, out_ref, sems):
    copies = []
    for b in range(N_LEV):
        copies.append(pltpu.make_async_copy(table_ref.at[own_slot(b)], out_ref.at[b, pl.ds(0, 20)], sems.at[2 * b]))
        half = table_ref.at[shared_slot(b), pl.ds(10 * (b & 1), 10)]
        copies.append(pltpu.make_async_copy(half, out_ref.at[b, pl.ds(20, 10)], sems.at[2 * b + 1]))
    for copy in copies:
        copy.start()
    for copy in copies:
        copy.wait()


def send_tables(legendre):
    return pl.pallas_call(
        send_kernel,
        out_shape=jax.ShapeDtypeStruct((N_LEV, 30, 2, HL), BF16),
        in_specs=[VM],
        out_specs=ANY,
        scratch_shapes=[pltpu.SemaphoreType.DMA((2 * N_LEV,))],
        name="send_tables",
        interpret=INTERPRET,
        cost_estimate=pl.CostEstimate(flops=10**6, bytes_accessed=2 * 10**6, transcendentals=0),
    )(jnp.swapaxes(legendre, 1, 2))


def received_tables(got):
    return got[:, :20].reshape(QP, HL), got[:, 20:].reshape(QP // 2, HL)


def exchange(value, axes):
    return lax.all_to_all(value, axes, split_axis=0, concat_axis=0, tiled=True)


def step_of(tracer, offsets, stencil, assign, legendre, damping, vert_vecs, vert_inv):
    lat = lax.axis_index("lat")
    side = lat & 1
    rows = jnp.swapaxes(tracer, 0, 1)
    near = lax.dynamic_slice_in_dim(rows, jnp.where(side == 1, 0, ROWS - 3), 3)
    near = lax.ppermute(near, "lat", [(i, i ^ 1) for i in range(N_LAT)])
    far = lax.dynamic_slice_in_dim(rows, jnp.where(side == 1, ROWS - 3, 0), 3)
    far = lax.ppermute(far, "lat", [(i, i + 2 * (i & 1) - 1) for i in range(1, N_LAT - 1)])
    table, even, weight = tables(assign)
    packed = send_tables(legendre)
    matrices = exchange(packed, "lev")
    own, shared = received_tables(matrices)
    msgs = forward(side.reshape(1), stencil, rows, near, far, jnp.swapaxes(offsets, 0, 1), table, even)
    got = exchange(msgs.reshape(N_DEV, 1, 128), ("lat", "lev")).reshape(N_DEV, 128)
    lev = lax.axis_index("lev")
    mine = lax.dynamic_slice_in_dim(assign, lat * SLOTS, SLOTS)
    info = jnp.stack([mine[own_slot(lev)], mine[shared_slot(lev)], lev & 1]).astype(jnp.int32)
    back, spec = spectral(
        info,
        got,
        own,
        shared,
        damping.reshape(32, 1),
        by_block(level_order(vert_inv, 1)),
        by_block(vert_vecs),
        by_block(level_order(vert_vecs, 0)),
    )
    home = exchange(back.reshape(N_DEV, 1, 128), ("lat", "lev")).reshape(N_DEV, 128)
    spec = exchange(spec, "lev")
    tracer_new = inverse(home, table, even, weight)
    spectral_new = place(spec).reshape(SLOTS, 20, 2, 64)
    return jnp.swapaxes(tracer_new, 0, 1), jnp.swapaxes(spectral_new, 1, 2)


def solution(mesh):
    placed = (
        P("lev", "lat", None),
        P(None, "lat", None),
        P(),
        P(),
        P("lat", None, "lev", None),
        P(),
        P(),
        P(),
    )
    return jax.shard_map(
        step_of,
        mesh=mesh,
        in_specs=placed,
        out_specs=(P("lev", "lat", None), P("lat", None, "lev", None)),
        check_vma=False,
    )
```

```python
import math

import jax
import jax.numpy as jnp
from jax import lax
from jax.experimental import pallas as pl
from jax.experimental.pallas import tpu as pltpu
from jax.sharding import PartitionSpec as P


INTERPRET = False
N_LAT, N_LEV = 32, 16
N_DEV = N_LAT * N_LEV
M = 640
NLON, HALF_LON = 1280, 640
ROWS = 20
LV = 2
QB = 40
QP = N_LEV * QB
HL = 320
SLOTS = 20
MSG = LV * ROWS
WIDE = 56
ZROW = 25
F32, BF16 = jnp.float32, jnp.bfloat16
NT = (((1,), (1,)), ((), ()))
NN = (((1,), (0,)), ((), ()))
HIGH = lax.Precision.HIGHEST


def own_slot(b):
    return 5 * (b >> 2) + (b & 3)


def shared_slot(b):
    return 5 * (b >> 2) + 4


def call(kernel, out_shape, in_specs, scratch, flops=10**7):
    many = isinstance(out_shape, (tuple, list))
    vm = pl.BlockSpec(memory_space=pltpu.VMEM)
    return pl.pallas_call(
        kernel,
        out_shape=out_shape,
        in_specs=in_specs,
        out_specs=[vm] * len(out_shape) if many else vm,
        scratch_shapes=scratch,
        interpret=INTERPRET,
        cost_estimate=pl.CostEstimate(flops=flops, bytes_accessed=10**6, transcendentals=0),
    )


VM = pl.BlockSpec(memory_space=pltpu.VMEM)
ANY = pl.BlockSpec(memory_space=pl.ANY)
SM = pl.BlockSpec(memory_space=pltpu.SMEM)


def cos_sin(phase):
    quad = jnp.floor((phase + 160.5) * (1.0 / 320.0))
    x = (phase - 320.0 * quad) * (2.0 * math.pi / NLON)
    z = x * x
    s = x * (1.0 + z * (-1.6666654611e-1 + z * (8.3321608736e-3 - z * 1.9515295891e-4)))
    c = 1.0 - 0.5 * z + z * z * (
        4.166664568298827e-2 + z * (-1.388731625493765e-3 + z * 2.443315711809948e-5)
    )
    odd = jnp.logical_or(quad == 1.0, quad == 3.0)
    c, s = jnp.where(odd, s, c), jnp.where(odd, c, s)
    c = jnp.where(jnp.logical_or(quad == 1.0, quad == 2.0), -c, c)
    s = jnp.where(jnp.logical_or(quad == 2.0, quad == 3.0), -s, s)
    return c, s


def wrapped(count):
    return count - NLON * jnp.floor((count + 0.5) * (1.0 / NLON))


CHUNK = 64


def tables_kernel(assign_ref, t_out, even_ref, weight_ref, t_ref, sems):
    def write(i):
        rows = pl.ds(pl.multiple_of(i * CHUNK, CHUNK), CHUNK)
        return pltpu.make_async_copy(t_ref.at[:, rows], t_out.at[:, rows], sems.at[i])

    slots = lax.broadcasted_iota(jnp.int32, (CHUNK, M), 1)
    lane = lax.broadcasted_iota(jnp.int32, (CHUNK, 128), 1)
    lane_f = lane.astype(F32)
    assign = assign_ref[...].reshape(1, M).astype(F32)

    def step(i, carry):
        r0 = pl.multiple_of(i * CHUNK, CHUNK)
        d = r0 + lax.broadcasted_iota(jnp.int32, (CHUNK, 1), 0)
        lev = d & 15
        waves, evens, weights = [], [], []
        for slot in (own_slot(lev), shared_slot(lev)):
            wave = jnp.sum(jnp.where(slots == (d >> 4) * SLOTS + slot, assign, 0.0), axis=1, keepdims=True)
            waves.append(wave)
            evens.append(jnp.where(wave == 2.0 * jnp.floor(wave * 0.5), 1.0, 0.0))
            weights.append(jnp.where(wave == 0.0, 1.0, 2.0))
        turn_c, turn_s = cos_sin(wrapped(jnp.where(lane == 0, waves[0], waves[1]) * 128.0))

        def put(j, block, value):
            high = value.astype(BF16)
            t_ref[j, pl.ds(r0, CHUNK), 128 * block : 128 * block + 128] = high
            low = (value - high.astype(F32)).astype(BF16)
            t_ref[j, pl.ds(r0, CHUNK), HALF_LON + 128 * block : HALF_LON + 128 * block + 128] = low

        for u in range(2):
            start = wrapped(waves[u] * lane_f + (jnp.where((lev & 2) == 2, 320.0, 0.0) if u else 0.0))
            c, s = cos_sin(start)
            c = c * (1.0 / math.sqrt(NLON))
            s = s * (1.0 / math.sqrt(NLON))
            cd, sd = turn_c[:, u : u + 1], turn_s[:, u : u + 1]
            for block in range(5):
                put(2 * u, block, c)
                if u == 0:
                    put(1, block, -s)
                if block < 4:
                    c, s = c * cd - s * sd, s * cd + c * sd
        even_ref[pl.ds(r0, CHUNK), :] = jnp.where(
            lane < 2 * MSG, evens[0], evens[1]
        )
        weight_ref[pl.ds(r0, CHUNK), :] = jnp.where(
            lane < 2 * MSG, weights[0], weights[1]
        )
        write(i).start()
        return carry

    lax.fori_loop(0, N_DEV // CHUNK, step, 0)
    for i in range(N_DEV // CHUNK):
        write(i).wait()


def tables(assign):
    return pl.pallas_call(
        tables_kernel,
        out_shape=(
            jax.ShapeDtypeStruct((3, N_DEV, NLON), BF16),
            jax.ShapeDtypeStruct((N_DEV, 128), F32),
            jax.ShapeDtypeStruct((N_DEV, 128), F32),
        ),
        in_specs=[VM],
        out_specs=(ANY, VM, VM),
        scratch_shapes=[pltpu.VMEM((3, N_DEV, NLON), BF16), pltpu.SemaphoreType.DMA((N_DEV // CHUNK,))],
        name="tables",
        interpret=INTERPRET,
        cost_estimate=pl.CostEstimate(flops=10**7, bytes_accessed=10**6, transcendentals=0),
    )(assign)


def forward_kernel(
    side_ref,
    stencil_ref,
    tracer_ref,
    near_ref,
    far_ref,
    off_ref,
    t_any,
    even_ref,
    out_ref,
    pad,
    rolled,
    codes,
    adv,
    fe,
    fo,
    t_ref,
    t_sem,
):
    fetch = pltpu.make_async_copy(t_any, t_ref, t_sem)
    fetch.start()
    odd_band = side_ref[0] == 1
    pad[...] = jnp.zeros((64, NLON), F32)
    for i in range(3):
        pad[2 + 2 * i : 4 + 2 * i, :] = jnp.where(odd_band, near_ref[i], far_ref[i])
        pad[48 + 2 * i : 50 + 2 * i, :] = jnp.where(odd_band, far_ref[i], near_ref[i])
    for i in range(ROWS):
        pad[8 + 2 * i : 10 + 2 * i, :] = tracer_ref[i]
        codes[2 * i : 2 * i + 2, :] = off_ref[i]
    for bi in range(7):
        shift = (3 - bi) % NLON
        rolled[bi] = pltpu.roll(pad[...], shift, 1) if shift else pad[...]

    first = (lax.broadcasted_iota(jnp.int32, (2 * ROWS, 128), 0) & 1) == 0

    def chunk(ci, carry):
        l0 = pl.multiple_of(ci * 128, 128)
        value = codes[:, pl.ds(l0, 128)]
        part = jnp.where(first, value * 7, value)
        code = part + jnp.where(first, jnp.roll(part, -1, 0), jnp.roll(part, 1, 0))
        acc = jnp.zeros((2 * ROWS, 128), F32)
        for ai in range(7):
            for bi in range(7):
                s = stencil_ref[ai, bi]
                w = jnp.where(code == (ai - 3) * 7 + (bi - 3), s + 1.0, s)
                acc = acc + w * rolled[bi, 2 + 2 * ai : 42 + 2 * ai, pl.ds(l0, 128)]
        adv[ci] = acc
        return carry

    lax.fori_loop(0, NLON // 128, chunk, 0)
    levels = [
        jnp.concatenate([every_other(adv, ci, k) for ci in range(NLON // 128)], axis=1) for k in range(LV)
    ]
    x = jnp.concatenate(
        [v[:, :HALF_LON] + v[:, HALF_LON:] for v in levels] + [v[:, :HALF_LON] - v[:, HALF_LON:] for v in levels], axis=0
    )
    high = x.astype(BF16)
    low = (x - high.astype(F32)).astype(BF16)
    right = jnp.concatenate(
        [
            jnp.concatenate([high, high], axis=1),
            jnp.concatenate([low, jnp.zeros_like(low)], axis=1),
        ],
        axis=0,
    )
    fe[...] = jnp.zeros((N_DEV, 128), F32)
    fo[...] = jnp.zeros((N_DEV, 128), F32)
    fetch.wait()
    for j in range(3):
        prod = lax.dot_general(t_ref[j], right, NT, preferred_element_type=F32)
        fe[:, MSG * j : MSG * (j + 1)] = prod[:, 0:MSG] + prod[:, 2 * MSG : 3 * MSG]
        fo[:, MSG * j : MSG * (j + 1)] = prod[:, MSG : 2 * MSG] + prod[:, 3 * MSG : 4 * MSG]
    out_ref[...] = jnp.where(even_ref[...] > 0.5, fe[...], fo[...])


def every_other(ref, ci, k):
    return ref[ci][k::2] if INTERPRET else ref[ci, pl.ds(k, ROWS, 2), :]


def forward(side, stencil, tracer, near, far, offsets, table, even):
    return call(
        forward_kernel,
        jax.ShapeDtypeStruct((N_DEV, 128), F32),
        [SM, SM, VM, VM, VM, VM, ANY, VM],
        [
            pltpu.VMEM((64, NLON), F32),
            pltpu.VMEM((7, 64, NLON), F32),
            pltpu.VMEM((2 * ROWS, NLON), jnp.int32),
            pltpu.VMEM((NLON // 128, 2 * ROWS, 128), F32),
            pltpu.VMEM((N_DEV, 128), F32),
            pltpu.VMEM((N_DEV, 128), F32),
            pltpu.VMEM((3, N_DEV, NLON), BF16),
            pltpu.SemaphoreType.DMA,
        ],
        10**9,
    )(side, stencil, tracer, near, far, offsets, table, even)


def mirror_matrix():
    src = lax.broadcasted_iota(jnp.int32, (128, 128), 0)
    dst = lax.broadcasted_iota(jnp.int32, (128, 128), 1)
    hit = jnp.zeros((128, 128), jnp.bool_)
    for g in range(6):
        hit = jnp.logical_or(
            hit, jnp.logical_and(jnp.logical_and(dst >= 20 * g, dst < 20 * g + 20), src + dst == 40 * g + 19)
        )
    return hit.astype(F32)


def spectral_kernel(
    info_ref,
    msg_ref,
    own_ref,
    shared_ref,
    damping_ref,
    inv_ref,
    vec_ref,
    vecp_ref,
    out_ref,
    nbuf,
    sbuf,
    flip,
    zonal,
    wide,
):
    mirror = mirror_matrix()
    half = N_DEV // 2
    flip[...] = lax.dot_general(msg_ref[half:, :], mirror, NN, precision=HIGH, preferred_element_type=F32)
    for a in range(N_LAT // 2):
        top = msg_ref[16 * a : 16 * a + 16, :]
        low = flip[16 * (15 - a) : 16 * (15 - a) + 16, :]
        for j in range(3):
            for k in range(LV):
                lane = MSG * j + ROWS * k
                nbuf[j, 16 * k : 16 * k + 16, ROWS * a : ROWS * a + ROWS] = top[:, lane : lane + ROWS]
                sbuf[j, 16 * k : 16 * k + 16, ROWS * a : ROWS * a + ROWS] = low[:, lane : lane + ROWS]
    damp = damping_ref[...]

    def exact(left, right):
        return lax.dot_general(left, right, NN, precision=HIGH, preferred_element_type=F32)

    def solve(units, matrix, degree, odd):
        count = len(units)
        hemi = jnp.concatenate(
            [part for j in units for part in (nbuf[j] + sbuf[j], nbuf[j] - sbuf[j])], axis=0
        ).astype(BF16)
        prod = lax.dot_general(hemi, matrix, NT, preferred_element_type=F32)
        keep = degree <= M - 1
        forcing = jnp.concatenate(
            [
                jnp.where(keep, jnp.where(odd, prod[64 * u + 32 : 64 * u + 64], prod[64 * u : 64 * u + 32]), 0.0)
                for u in range(count)
            ],
            axis=0,
        )
        size = 32 * count
        n = degree.astype(F32)
        denominator = 1.0 + (n * (n + 1.0) / float(M * M)) * damp
        modal = exact(inv_ref[:size, :size], forcing)
        modal = jnp.concatenate([modal[32 * u : 32 * u + 32] / denominator for u in range(count)], axis=0)
        packed = exact(vecp_ref[:size, :size], modal)
        left = jnp.concatenate(
            [
                part
                for u in range(count)
                for part in (
                    packed[32 * u : 32 * u + 32],
                    jnp.where(odd, -packed[32 * u : 32 * u + 32], packed[32 * u : 32 * u + 32]),
                )
            ],
            axis=0,
        ).astype(BF16)
        back = lax.dot_general(left, matrix, NN, preferred_element_type=F32)
        for u, j in enumerate(units):
            lats = jnp.concatenate([back[64 * u : 64 * u + 32], back[64 * u + 32 : 64 * u + 64]], axis=1)
            for tile in range(5):
                zonal[tile, 32 * j : 32 * j + 32, :] = lats[:, 128 * tile : 128 * tile + 128]
        return exact(vec_ref[:size, :size], modal).T

    lane = lax.broadcasted_iota(jnp.int32, (32, QP), 1)
    whole = solve((0, 1), own_ref[...], lane + info_ref[0], (lane & 1) == 1)
    lane = lax.broadcasted_iota(jnp.int32, (32, QP // 2), 1)
    block = jnp.floor((lane.astype(F32) + 0.5) * (1.0 / 20.0)).astype(jnp.int32)
    part = solve((2,), shared_ref[...], lane + 20 * block + 20 * info_ref[2] + info_ref[1], (lane & 1) == 1)
    for b in range(N_LEV):
        wide[b, 0:20, 0:64] = whole[QB * b : QB * b + 20]
        wide[b, 0:20, 64:128] = whole[QB * b + 20 : QB * b + 40]
        for g in range(4):
            wide[b, 20:25, 32 * g : 32 * g + 32] = part[20 * b + 5 * g : 20 * b + 5 * g + 5]
        for tile in range(5):
            wide[b, ZROW + 6 * tile : ZROW + 6 * tile + 6, :] = strided(zonal, tile, b, 6, 16)
        wide[b, ZROW + 30 : WIDE, :] = jnp.zeros((WIDE - ZROW - 30, 128), F32)
    out_ref[...] = wide[...].astype(BF16)


def strided(ref, tile, start, count, stride):
    if INTERPRET:
        return ref[tile][start :: stride][:count]
    return ref[tile, pl.ds(start, count, stride), :]


def spectral(info, msgs, own, shared, damping, inv, vec, vecp):
    return call(
        spectral_kernel,
        jax.ShapeDtypeStruct((N_LEV, WIDE, 128), BF16),
        [SM, VM, VM, VM, VM, VM, VM, VM],
        [
            pltpu.VMEM((3, 32, HL), F32),
            pltpu.VMEM((3, 32, HL), F32),
            pltpu.VMEM((N_DEV // 2, 128), F32),
            pltpu.VMEM((5, 96, 128), F32),
            pltpu.VMEM((N_LEV, WIDE, 128), F32),
        ],
        10**9,
    )(info, msgs, own, shared, damping, inv, vec, vecp)


def bands_kernel(wide_ref, out_ref, rows, out, flip):
    half = N_DEV // 2
    for b in range(N_LEV):
        value = wide_ref[b].astype(F32)
        for tile in range(5):
            rows[tile, 8 * b : 8 * b + 6, :] = value[ZROW + 6 * tile : ZROW + 6 * tile + 6]
    out[...] = jnp.zeros((half, 128), F32)
    flip[...] = jnp.zeros((half, 128), F32)
    for j in range(3):
        for k in range(LV):
            lane = MSG * j + ROWS * k
            lats = jnp.concatenate([strided(rows, tile, LV * j + k, N_LEV, 8) for tile in range(5)], axis=1)
            for a in range(N_LAT // 2):
                out[16 * a : 16 * a + 16, lane : lane + ROWS] = lats[:, ROWS * a : ROWS * a + ROWS]
                flip[16 * (15 - a) : 16 * (15 - a) + 16, lane : lane + ROWS] = lats[:, HL + ROWS * a : HL + ROWS * a + ROWS]
    mirror = mirror_matrix().astype(BF16)
    low = lax.dot_general(flip[...].astype(BF16), mirror, NN, preferred_element_type=F32)
    out_ref[:half, :] = out[...].astype(BF16)
    out_ref[half:, :] = low.astype(BF16)


def bands(wide):
    return call(
        bands_kernel,
        jax.ShapeDtypeStruct((N_DEV, 128), BF16),
        [VM],
        [
            pltpu.VMEM((5, 8 * N_LEV, 128), F32),
            pltpu.VMEM((N_DEV // 2, 128), F32),
            pltpu.VMEM((N_DEV // 2, 128), F32),
        ],
        10**7,
    )(wide)


def inverse_kernel(msg_ref, t_any, even_ref, weight_ref, out_ref, t_ref, t_sem):
    fetch = pltpu.make_async_copy(t_any.at[:, :, pl.ds(0, HALF_LON)], t_ref, t_sem)
    fetch.start()
    lane = lax.broadcasted_iota(jnp.int32, (N_DEV, 128), 1)
    scaled = jnp.where(lane < 3 * MSG, msg_ref[...].astype(F32) * weight_ref[...], 0.0)
    even = (scaled * even_ref[...]).T
    odd = (scaled * (1.0 - even_ref[...])).T
    total = jnp.zeros((2 * MSG, HALF_LON), F32)
    fetch.wait()
    for j in range(3):
        left = jnp.concatenate([even[MSG * j : MSG * (j + 1)], odd[MSG * j : MSG * (j + 1)]], axis=0).astype(BF16)
        total = total + lax.dot_general(left, t_ref[j], NN, preferred_element_type=F32)
    near = total[:MSG] + total[MSG:]
    far = total[:MSG] - total[MSG:]
    for k in range(LV):
        out_ref[:, k, :HALF_LON] = near[ROWS * k : ROWS * (k + 1)]
        out_ref[:, k, HALF_LON:] = far[ROWS * k : ROWS * (k + 1)]


def inverse(msgs, table, even, weight):
    return call(
        inverse_kernel,
        jax.ShapeDtypeStruct((ROWS, LV, NLON), F32),
        [VM, ANY, VM, VM],
        [pltpu.VMEM((3, N_DEV, HALF_LON), BF16), pltpu.SemaphoreType.DMA],
        10**8,
    )(msgs, table, even, weight)


def place_kernel(spec_ref, out_ref):
    for b in range(N_LEV):
        c, half = (b & 3) >> 1, b & 1
        value = spec_ref[b].astype(F32)
        out_ref[own_slot(b), 0:20, :] = value[0:20, 0:64]
        out_ref[own_slot(b), 20:40, :] = value[0:20, 64:128]
        for g in range(4):
            first = 20 * half + 5 * g
            out_ref[shared_slot(b), first : first + 5, 32 * c : 32 * c + 32] = value[20:25, 32 * g : 32 * g + 32]


def place(spec):
    return call(place_kernel, jax.ShapeDtypeStruct((SLOTS, QB, 64), F32), [VM], [], 10**6)(spec)


def by_block(matrix):
    return jnp.kron(jnp.eye(2, dtype=F32), matrix)


def level_order(value, axis):
    shape = value.shape
    split = shape[:axis] + (16, 2) + shape[axis + 1 :]
    return jnp.swapaxes(value.reshape(split), axis, axis + 1).reshape(shape)


def send_kernel(table_ref, out_ref, sems):
    copies = []
    for b in range(N_LEV):
        copies.append(pltpu.make_async_copy(table_ref.at[own_slot(b)], out_ref.at[b, pl.ds(0, 20)], sems.at[2 * b]))
        half = table_ref.at[shared_slot(b), pl.ds(10 * (b & 1), 10)]
        copies.append(pltpu.make_async_copy(half, out_ref.at[b, pl.ds(20, 10)], sems.at[2 * b + 1]))
    for copy in copies:
        copy.start()
    for copy in copies:
        copy.wait()


def send_tables(legendre):
    return pl.pallas_call(
        send_kernel,
        out_shape=jax.ShapeDtypeStruct((N_LEV, 30, 2, HL), BF16),
        in_specs=[VM],
        out_specs=ANY,
        scratch_shapes=[pltpu.SemaphoreType.DMA((2 * N_LEV,))],
        name="send_tables",
        interpret=INTERPRET,
        cost_estimate=pl.CostEstimate(flops=10**6, bytes_accessed=2 * 10**6, transcendentals=0),
    )(jnp.swapaxes(legendre, 1, 2))


def received_tables(got):
    return got[:, :20].reshape(QP, HL), got[:, 20:].reshape(QP // 2, HL)


def exchange(value, axes):
    return lax.all_to_all(value, axes, split_axis=0, concat_axis=0, tiled=True)


def step_of(tracer, offsets, stencil, assign, legendre, damping, vert_vecs, vert_inv):
    lat = lax.axis_index("lat")
    side = lat & 1
    rows = jnp.swapaxes(tracer, 0, 1)
    near = lax.dynamic_slice_in_dim(rows, jnp.where(side == 1, 0, ROWS - 3), 3)
    near = lax.ppermute(near, "lat", [(i, i ^ 1) for i in range(N_LAT)])
    far = lax.dynamic_slice_in_dim(rows, jnp.where(side == 1, ROWS - 3, 0), 3)
    far = lax.ppermute(far, "lat", [(i, i + 2 * (i & 1) - 1) for i in range(1, N_LAT - 1)])
    table, even, weight = tables(assign)
    packed = send_tables(legendre)
    matrices = exchange(packed, "lev")
    own, shared = received_tables(matrices)
    msgs = forward(side.reshape(1), stencil, rows, near, far, jnp.swapaxes(offsets, 0, 1), table, even)
    got = exchange(msgs.reshape(N_DEV, 1, 128), ("lat", "lev")).reshape(N_DEV, 128)
    lev = lax.axis_index("lev")
    mine = lax.dynamic_slice_in_dim(assign, lat * SLOTS, SLOTS)
    info = jnp.stack([mine[own_slot(lev)], mine[shared_slot(lev)], lev & 1]).astype(jnp.int32)
    solved = spectral(
        info,
        got,
        own,
        shared,
        damping.reshape(32, 1),
        by_block(level_order(vert_inv, 1)),
        by_block(vert_vecs),
        by_block(level_order(vert_vecs, 0)),
    )
    solved = exchange(solved, "lev")
    home = exchange(bands(solved).reshape(N_LAT, N_LEV, 128), "lat").reshape(N_DEV, 128)
    tracer_new = inverse(home, table, even, weight)
    spectral_new = place(solved).reshape(SLOTS, 20, 2, 64)
    return jnp.swapaxes(tracer_new, 0, 1), jnp.swapaxes(spectral_new, 1, 2)


def solution(mesh):
    placed = (
        P("lev", "lat", None),
        P(None, "lat", None),
        P(),
        P(),
        P("lat", None, "lev", None),
        P(),
        P(),
        P(),
    )
    return jax.shard_map(
        step_of,
        mesh=mesh,
        in_specs=placed,
        out_specs=(P("lev", "lat", None), P("lat", None, "lev", None)),
        check_vma=False,
    )
```

```python
import math

import jax
import jax.numpy as jnp
from jax import lax
from jax.experimental import pallas as pl
from jax.experimental.pallas import tpu as pltpu
from jax.sharding import PartitionSpec as P


INTERPRET = False
N_LAT, N_LEV = 32, 16
N_DEV = N_LAT * N_LEV
M = 640
NLON, HALF_LON = 1280, 640
ROWS = 20
LV = 2
QB = 40
QP = N_LEV * QB
HL = 320
SLOTS = 20
MSG = LV * ROWS
WIDE = 56
ZROW = 25
F32, BF16 = jnp.float32, jnp.bfloat16
NT = (((1,), (1,)), ((), ()))
NN = (((1,), (0,)), ((), ()))
HIGH = lax.Precision.HIGHEST


def own_slot(b):
    return 5 * (b >> 2) + (b & 3)


def shared_slot(b):
    return 5 * (b >> 2) + 4


def call(kernel, out_shape, in_specs, scratch, flops=10**7):
    many = isinstance(out_shape, (tuple, list))
    vm = pl.BlockSpec(memory_space=pltpu.VMEM)
    return pl.pallas_call(
        kernel,
        out_shape=out_shape,
        in_specs=in_specs,
        out_specs=[vm] * len(out_shape) if many else vm,
        scratch_shapes=scratch,
        interpret=INTERPRET,
        cost_estimate=pl.CostEstimate(flops=flops, bytes_accessed=10**6, transcendentals=0),
    )


VM = pl.BlockSpec(memory_space=pltpu.VMEM)
ANY = pl.BlockSpec(memory_space=pl.ANY)
SM = pl.BlockSpec(memory_space=pltpu.SMEM)


def cos_sin(phase):
    quad = jnp.floor((phase + 160.5) * (1.0 / 320.0))
    x = (phase - 320.0 * quad) * (2.0 * math.pi / NLON)
    z = x * x
    s = x * (1.0 + z * (-1.6666654611e-1 + z * (8.3321608736e-3 - z * 1.9515295891e-4)))
    c = 1.0 - 0.5 * z + z * z * (
        4.166664568298827e-2 + z * (-1.388731625493765e-3 + z * 2.443315711809948e-5)
    )
    odd = jnp.logical_or(quad == 1.0, quad == 3.0)
    c, s = jnp.where(odd, s, c), jnp.where(odd, c, s)
    c = jnp.where(jnp.logical_or(quad == 1.0, quad == 2.0), -c, c)
    s = jnp.where(jnp.logical_or(quad == 2.0, quad == 3.0), -s, s)
    return c, s


def wrapped(count):
    return count - NLON * jnp.floor((count + 0.5) * (1.0 / NLON))


CHUNK = 64


def tables_kernel(assign_ref, t_out, even_ref, weight_ref, t_ref, sems):
    def write(i):
        rows = pl.ds(pl.multiple_of(i * CHUNK, CHUNK), CHUNK)
        return pltpu.make_async_copy(t_ref.at[:, rows], t_out.at[:, rows], sems.at[i])

    slots = lax.broadcasted_iota(jnp.int32, (CHUNK, M), 1)
    lane = lax.broadcasted_iota(jnp.int32, (CHUNK, 128), 1)
    lane_f = lane.astype(F32)
    assign = assign_ref[...].reshape(1, M).astype(F32)

    def step(i, carry):
        r0 = pl.multiple_of(i * CHUNK, CHUNK)
        d = r0 + lax.broadcasted_iota(jnp.int32, (CHUNK, 1), 0)
        lev = d & 15
        waves, evens, weights = [], [], []
        for slot in (own_slot(lev), shared_slot(lev)):
            wave = jnp.sum(jnp.where(slots == (d >> 4) * SLOTS + slot, assign, 0.0), axis=1, keepdims=True)
            waves.append(wave)
            evens.append(jnp.where(wave == 2.0 * jnp.floor(wave * 0.5), 1.0, 0.0))
            weights.append(jnp.where(wave == 0.0, 1.0, 2.0))
        turn_c, turn_s = cos_sin(wrapped(jnp.where(lane == 0, waves[0], waves[1]) * 128.0))

        def put(j, block, value):
            high = value.astype(BF16)
            t_ref[j, pl.ds(r0, CHUNK), 128 * block : 128 * block + 128] = high
            low = (value - high.astype(F32)).astype(BF16)
            t_ref[j, pl.ds(r0, CHUNK), HALF_LON + 128 * block : HALF_LON + 128 * block + 128] = low

        for u in range(2):
            start = wrapped(waves[u] * lane_f + (jnp.where((lev & 2) == 2, 320.0, 0.0) if u else 0.0))
            c, s = cos_sin(start)
            c = c * (1.0 / math.sqrt(NLON))
            s = s * (1.0 / math.sqrt(NLON))
            cd, sd = turn_c[:, u : u + 1], turn_s[:, u : u + 1]
            for block in range(5):
                put(2 * u, block, c)
                if u == 0:
                    put(1, block, -s)
                if block < 4:
                    c, s = c * cd - s * sd, s * cd + c * sd
        even_ref[pl.ds(r0, CHUNK), :] = jnp.where(
            lane < 2 * MSG, evens[0], evens[1]
        )
        weight_ref[pl.ds(r0, CHUNK), :] = jnp.where(
            lane < 2 * MSG, weights[0], weights[1]
        )
        write(i).start()
        return carry

    lax.fori_loop(0, N_DEV // CHUNK, step, 0)
    for i in range(N_DEV // CHUNK):
        write(i).wait()


def tables(assign):
    return pl.pallas_call(
        tables_kernel,
        out_shape=(
            jax.ShapeDtypeStruct((3, N_DEV, NLON), BF16),
            jax.ShapeDtypeStruct((N_DEV, 128), F32),
            jax.ShapeDtypeStruct((N_DEV, 128), F32),
        ),
        in_specs=[VM],
        out_specs=(ANY, VM, VM),
        scratch_shapes=[pltpu.VMEM((3, N_DEV, NLON), BF16), pltpu.SemaphoreType.DMA((N_DEV // CHUNK,))],
        name="tables",
        interpret=INTERPRET,
        cost_estimate=pl.CostEstimate(flops=10**7, bytes_accessed=10**6, transcendentals=0),
    )(assign)


def forward_kernel(
    side_ref,
    stencil_ref,
    tracer_ref,
    near_ref,
    far_ref,
    off_ref,
    t_any,
    even_ref,
    out_ref,
    pad,
    rolled,
    codes,
    adv,
    fe,
    fo,
    t_ref,
    t_sem,
):
    fetch = pltpu.make_async_copy(t_any, t_ref, t_sem)
    fetch.start()
    odd_band = side_ref[0] == 1
    pad[...] = jnp.zeros((64, NLON), F32)
    for i in range(3):
        pad[2 + 2 * i : 4 + 2 * i, :] = jnp.where(odd_band, near_ref[i], far_ref[i])
        pad[48 + 2 * i : 50 + 2 * i, :] = jnp.where(odd_band, far_ref[i], near_ref[i])
    for i in range(ROWS):
        pad[8 + 2 * i : 10 + 2 * i, :] = tracer_ref[i]
        codes[2 * i : 2 * i + 2, :] = off_ref[i]
    for bi in range(7):
        shift = (3 - bi) % NLON
        rolled[bi] = pltpu.roll(pad[...], shift, 1) if shift else pad[...]

    first = (lax.broadcasted_iota(jnp.int32, (2 * ROWS, 128), 0) & 1) == 0

    def chunk(ci, carry):
        l0 = pl.multiple_of(ci * 128, 128)
        value = codes[:, pl.ds(l0, 128)]
        part = jnp.where(first, value * 7, value)
        code = part + jnp.where(first, jnp.roll(part, -1, 0), jnp.roll(part, 1, 0))
        acc = jnp.zeros((2 * ROWS, 128), F32)
        for ai in range(7):
            for bi in range(7):
                s = stencil_ref[ai, bi]
                w = jnp.where(code == (ai - 3) * 7 + (bi - 3), s + 1.0, s)
                acc = acc + w * rolled[bi, 2 + 2 * ai : 42 + 2 * ai, pl.ds(l0, 128)]
        adv[ci] = acc
        return carry

    lax.fori_loop(0, NLON // 128, chunk, 0)
    levels = [
        jnp.concatenate([every_other(adv, ci, k) for ci in range(NLON // 128)], axis=1) for k in range(LV)
    ]
    x = jnp.concatenate(
        [v[:, :HALF_LON] + v[:, HALF_LON:] for v in levels] + [v[:, :HALF_LON] - v[:, HALF_LON:] for v in levels], axis=0
    )
    high = x.astype(BF16)
    low = (x - high.astype(F32)).astype(BF16)
    right = jnp.concatenate(
        [
            jnp.concatenate([high, high], axis=1),
            jnp.concatenate([low, jnp.zeros_like(low)], axis=1),
        ],
        axis=0,
    )
    fe[...] = jnp.zeros((N_DEV, 128), F32)
    fo[...] = jnp.zeros((N_DEV, 128), F32)
    fetch.wait()
    for j in range(3):
        prod = lax.dot_general(t_ref[j], right, NT, preferred_element_type=F32)
        fe[:, MSG * j : MSG * (j + 1)] = prod[:, 0:MSG] + prod[:, 2 * MSG : 3 * MSG]
        fo[:, MSG * j : MSG * (j + 1)] = prod[:, MSG : 2 * MSG] + prod[:, 3 * MSG : 4 * MSG]
    out_ref[...] = jnp.where(even_ref[...] > 0.5, fe[...], fo[...])


def every_other(ref, ci, k):
    return ref[ci][k::2] if INTERPRET else ref[ci, pl.ds(k, ROWS, 2), :]


def forward(side, stencil, tracer, near, far, offsets, table, even):
    return call(
        forward_kernel,
        jax.ShapeDtypeStruct((N_DEV, 128), F32),
        [SM, SM, VM, VM, VM, VM, ANY, VM],
        [
            pltpu.VMEM((64, NLON), F32),
            pltpu.VMEM((7, 64, NLON), F32),
            pltpu.VMEM((2 * ROWS, NLON), jnp.int32),
            pltpu.VMEM((NLON // 128, 2 * ROWS, 128), F32),
            pltpu.VMEM((N_DEV, 128), F32),
            pltpu.VMEM((N_DEV, 128), F32),
            pltpu.VMEM((3, N_DEV, NLON), BF16),
            pltpu.SemaphoreType.DMA,
        ],
        10**9,
    )(side, stencil, tracer, near, far, offsets, table, even)


def mirror_matrix():
    src = lax.broadcasted_iota(jnp.int32, (128, 128), 0)
    dst = lax.broadcasted_iota(jnp.int32, (128, 128), 1)
    hit = jnp.zeros((128, 128), jnp.bool_)
    for g in range(6):
        hit = jnp.logical_or(
            hit, jnp.logical_and(jnp.logical_and(dst >= 20 * g, dst < 20 * g + 20), src + dst == 40 * g + 19)
        )
    return hit.astype(F32)


def spectral_kernel(
    info_ref,
    msg_ref,
    own_ref,
    shared_ref,
    damping_ref,
    inv_ref,
    vec_ref,
    vecp_ref,
    out_ref,
    nbuf,
    sbuf,
    flip,
    zonal,
    wide,
):
    mirror = mirror_matrix()
    half = N_DEV // 2
    flip[...] = lax.dot_general(msg_ref[half:, :], mirror, NN, precision=HIGH, preferred_element_type=F32)
    for a in range(N_LAT // 2):
        top = msg_ref[16 * a : 16 * a + 16, :]
        low = flip[16 * (15 - a) : 16 * (15 - a) + 16, :]
        for j in range(3):
            for k in range(LV):
                lane = MSG * j + ROWS * k
                nbuf[j, 16 * k : 16 * k + 16, ROWS * a : ROWS * a + ROWS] = top[:, lane : lane + ROWS]
                sbuf[j, 16 * k : 16 * k + 16, ROWS * a : ROWS * a + ROWS] = low[:, lane : lane + ROWS]
    damp = damping_ref[...]

    def exact(left, right):
        return lax.dot_general(left, right, NN, precision=HIGH, preferred_element_type=F32)

    def solve(units, matrix, degree, odd):
        count = len(units)
        hemi = jnp.concatenate(
            [part for j in units for part in (nbuf[j] + sbuf[j], nbuf[j] - sbuf[j])], axis=0
        ).astype(BF16)
        prod = lax.dot_general(hemi, matrix, NT, preferred_element_type=F32)
        keep = degree <= M - 1
        forcing = jnp.concatenate(
            [
                jnp.where(keep, jnp.where(odd, prod[64 * u + 32 : 64 * u + 64], prod[64 * u : 64 * u + 32]), 0.0)
                for u in range(count)
            ],
            axis=0,
        )
        size = 32 * count
        n = degree.astype(F32)
        denominator = 1.0 + (n * (n + 1.0) / float(M * M)) * damp
        modal = exact(inv_ref[:size, :size], forcing)
        modal = jnp.concatenate([modal[32 * u : 32 * u + 32] / denominator for u in range(count)], axis=0)
        packed = exact(vecp_ref[:size, :size], modal)
        left = jnp.concatenate(
            [
                part
                for u in range(count)
                for part in (
                    packed[32 * u : 32 * u + 32],
                    jnp.where(odd, -packed[32 * u : 32 * u + 32], packed[32 * u : 32 * u + 32]),
                )
            ],
            axis=0,
        ).astype(BF16)
        back = lax.dot_general(left, matrix, NN, preferred_element_type=F32)
        for u, j in enumerate(units):
            lats = jnp.concatenate([back[64 * u : 64 * u + 32], back[64 * u + 32 : 64 * u + 64]], axis=1)
            for tile in range(5):
                zonal[tile, 32 * j : 32 * j + 32, :] = lats[:, 128 * tile : 128 * tile + 128]
        return exact(vec_ref[:size, :size], modal).T

    lane = lax.broadcasted_iota(jnp.int32, (32, QP), 1)
    whole = solve((0, 1), own_ref[...], lane + info_ref[0], (lane & 1) == 1)
    lane = lax.broadcasted_iota(jnp.int32, (32, QP // 2), 1)
    block = jnp.floor((lane.astype(F32) + 0.5) * (1.0 / 20.0)).astype(jnp.int32)
    part = solve((2,), shared_ref[...], lane + 20 * block + 20 * info_ref[2] + info_ref[1], (lane & 1) == 1)
    for b in range(N_LEV):
        wide[b, 0:20, 0:64] = whole[QB * b : QB * b + 20]
        wide[b, 0:20, 64:128] = whole[QB * b + 20 : QB * b + 40]
        for g in range(4):
            wide[b, 20:25, 32 * g : 32 * g + 32] = part[20 * b + 5 * g : 20 * b + 5 * g + 5]
        for tile in range(5):
            wide[b, ZROW + 6 * tile : ZROW + 6 * tile + 6, :] = strided(zonal, tile, b, 6, 16)
        wide[b, ZROW + 30 : WIDE, :] = jnp.zeros((WIDE - ZROW - 30, 128), F32)
    out_ref[...] = wide[...].astype(BF16)


def strided(ref, tile, start, count, stride):
    if INTERPRET:
        return ref[tile][start :: stride][:count]
    return ref[tile, pl.ds(start, count, stride), :]


def spectral(info, msgs, own, shared, damping, inv, vec, vecp):
    return call(
        spectral_kernel,
        jax.ShapeDtypeStruct((N_LEV, WIDE, 128), BF16),
        [SM, VM, VM, VM, VM, VM, VM, VM],
        [
            pltpu.VMEM((3, 32, HL), F32),
            pltpu.VMEM((3, 32, HL), F32),
            pltpu.VMEM((N_DEV // 2, 128), F32),
            pltpu.VMEM((5, 96, 128), F32),
            pltpu.VMEM((N_LEV, WIDE, 128), F32),
        ],
        10**9,
    )(info, msgs, own, shared, damping, inv, vec, vecp)


def bands_kernel(wide_ref, out_ref, rows, out, flip):
    half = N_DEV // 2
    for b in range(N_LEV):
        value = wide_ref[b].astype(F32)
        for tile in range(5):
            rows[tile, 8 * b : 8 * b + 6, :] = value[ZROW + 6 * tile : ZROW + 6 * tile + 6]
    out[...] = jnp.zeros((half, 128), F32)
    flip[...] = jnp.zeros((half, 128), F32)
    for j in range(3):
        for k in range(LV):
            lane = MSG * j + ROWS * k
            lats = jnp.concatenate([strided(rows, tile, LV * j + k, N_LEV, 8) for tile in range(5)], axis=1)
            for a in range(N_LAT // 2):
                out[16 * a : 16 * a + 16, lane : lane + ROWS] = lats[:, ROWS * a : ROWS * a + ROWS]
                flip[16 * (15 - a) : 16 * (15 - a) + 16, lane : lane + ROWS] = lats[:, HL + ROWS * a : HL + ROWS * a + ROWS]
    mirror = mirror_matrix().astype(BF16)
    low = lax.dot_general(flip[...].astype(BF16), mirror, NN, preferred_element_type=F32)
    out_ref[:half, :] = out[...].astype(BF16)
    out_ref[half:, :] = low.astype(BF16)


def bands(wide):
    return call(
        bands_kernel,
        jax.ShapeDtypeStruct((N_DEV, 128), BF16),
        [VM],
        [
            pltpu.VMEM((5, 8 * N_LEV, 128), F32),
            pltpu.VMEM((N_DEV // 2, 128), F32),
            pltpu.VMEM((N_DEV // 2, 128), F32),
        ],
        10**7,
    )(wide)


def inverse_kernel(msg_ref, t_any, even_ref, weight_ref, out_ref, t_ref, t_sem):
    fetches = [
        pltpu.make_async_copy(t_any.at[j, :, pl.ds(0, HALF_LON)], t_ref.at[j], t_sem.at[j]) for j in range(3)
    ]
    for fetch in fetches:
        fetch.start()
    lane = lax.broadcasted_iota(jnp.int32, (N_DEV, 128), 1)
    scaled = jnp.where(lane < 3 * MSG, msg_ref[...].astype(F32) * weight_ref[...], 0.0)
    even = (scaled * even_ref[...]).T
    odd = (scaled * (1.0 - even_ref[...])).T
    total = jnp.zeros((2 * MSG, HALF_LON), F32)
    for j in range(3):
        fetches[j].wait()
        left = jnp.concatenate([even[MSG * j : MSG * (j + 1)], odd[MSG * j : MSG * (j + 1)]], axis=0).astype(BF16)
        total = total + lax.dot_general(left, t_ref[j], NN, preferred_element_type=F32)
    near = total[:MSG] + total[MSG:]
    far = total[:MSG] - total[MSG:]
    for k in range(LV):
        out_ref[:, k, :HALF_LON] = near[ROWS * k : ROWS * (k + 1)]
        out_ref[:, k, HALF_LON:] = far[ROWS * k : ROWS * (k + 1)]


def inverse(msgs, table, even, weight):
    return call(
        inverse_kernel,
        jax.ShapeDtypeStruct((ROWS, LV, NLON), F32),
        [VM, ANY, VM, VM],
        [pltpu.VMEM((3, N_DEV, HALF_LON), BF16), pltpu.SemaphoreType.DMA((3,))],
        10**8,
    )(msgs, table, even, weight)


def place_kernel(spec_ref, out_ref):
    for b in range(N_LEV):
        c, half = (b & 3) >> 1, b & 1
        value = spec_ref[b].astype(F32)
        out_ref[own_slot(b), 0:20, :] = value[0:20, 0:64]
        out_ref[own_slot(b), 20:40, :] = value[0:20, 64:128]
        for g in range(4):
            first = 20 * half + 5 * g
            out_ref[shared_slot(b), first : first + 5, 32 * c : 32 * c + 32] = value[20:25, 32 * g : 32 * g + 32]


def place(spec):
    return call(place_kernel, jax.ShapeDtypeStruct((SLOTS, QB, 64), F32), [VM], [], 10**6)(spec)


def by_block(matrix):
    return jnp.kron(jnp.eye(2, dtype=F32), matrix)


def level_order(value, axis):
    shape = value.shape
    split = shape[:axis] + (16, 2) + shape[axis + 1 :]
    return jnp.swapaxes(value.reshape(split), axis, axis + 1).reshape(shape)


def send_kernel(table_ref, out_ref, sems):
    copies = []
    for b in range(N_LEV):
        copies.append(pltpu.make_async_copy(table_ref.at[own_slot(b)], out_ref.at[b, pl.ds(0, 20)], sems.at[2 * b]))
        half = table_ref.at[shared_slot(b), pl.ds(10 * (b & 1), 10)]
        copies.append(pltpu.make_async_copy(half, out_ref.at[b, pl.ds(20, 10)], sems.at[2 * b + 1]))
    for copy in copies:
        copy.start()
    for copy in copies:
        copy.wait()


def send_tables(legendre):
    return pl.pallas_call(
        send_kernel,
        out_shape=jax.ShapeDtypeStruct((N_LEV, 30, 2, HL), BF16),
        in_specs=[VM],
        out_specs=ANY,
        scratch_shapes=[pltpu.SemaphoreType.DMA((2 * N_LEV,))],
        name="send_tables",
        interpret=INTERPRET,
        cost_estimate=pl.CostEstimate(flops=10**6, bytes_accessed=2 * 10**6, transcendentals=0),
    )(jnp.swapaxes(legendre, 1, 2))


def received_tables(got):
    return got[:, :20].reshape(QP, HL), got[:, 20:].reshape(QP // 2, HL)


def exchange(value, axes):
    return lax.all_to_all(value, axes, split_axis=0, concat_axis=0, tiled=True)


def step_of(tracer, offsets, stencil, assign, legendre, damping, vert_vecs, vert_inv):
    lat = lax.axis_index("lat")
    side = lat & 1
    rows = jnp.swapaxes(tracer, 0, 1)
    near = lax.dynamic_slice_in_dim(rows, jnp.where(side == 1, 0, ROWS - 3), 3)
    near = lax.ppermute(near, "lat", [(i, i ^ 1) for i in range(N_LAT)])
    far = lax.dynamic_slice_in_dim(rows, jnp.where(side == 1, ROWS - 3, 0), 3)
    far = lax.ppermute(far, "lat", [(i, i + 2 * (i & 1) - 1) for i in range(1, N_LAT - 1)])
    table, even, weight = tables(assign)
    packed = send_tables(legendre)
    matrices = exchange(packed, "lev")
    own, shared = received_tables(matrices)
    msgs = forward(side.reshape(1), stencil, rows, near, far, jnp.swapaxes(offsets, 0, 1), table, even)
    got = exchange(msgs.reshape(N_DEV, 1, 128), ("lat", "lev")).reshape(N_DEV, 128)
    lev = lax.axis_index("lev")
    mine = lax.dynamic_slice_in_dim(assign, lat * SLOTS, SLOTS)
    info = jnp.stack([mine[own_slot(lev)], mine[shared_slot(lev)], lev & 1]).astype(jnp.int32)
    solved = spectral(
        info,
        got,
        own,
        shared,
        damping.reshape(32, 1),
        by_block(level_order(vert_inv, 1)),
        by_block(vert_vecs),
        by_block(level_order(vert_vecs, 0)),
    )
    solved = exchange(solved, "lev")
    home = exchange(bands(solved).reshape(N_LAT, N_LEV, 128), "lat").reshape(N_DEV, 128)
    tracer_new = inverse(home, table, even, weight)
    spectral_new = place(solved).reshape(SLOTS, 20, 2, 64)
    return jnp.swapaxes(tracer_new, 0, 1), jnp.swapaxes(spectral_new, 1, 2)


def solution(mesh):
    placed = (
        P("lev", "lat", None),
        P(None, "lat", None),
        P(),
        P(),
        P("lat", None, "lev", None),
        P(),
        P(),
        P(),
    )
    return jax.shard_map(
        step_of,
        mesh=mesh,
        in_specs=placed,
        out_specs=(P("lev", "lat", None), P("lat", None, "lev", None)),
        check_vma=False,
    )
```

```python
import math

import jax
import jax.numpy as jnp
from jax import lax
from jax.experimental import pallas as pl
from jax.experimental.pallas import tpu as pltpu
from jax.sharding import PartitionSpec as P


INTERPRET = False
N_LAT, N_LEV = 32, 16
N_DEV = N_LAT * N_LEV
M = 640
NLON, HALF_LON = 1280, 640
ROWS = 20
LV = 2
NLEV = 32
QB = 40
QP = N_LEV * QB
HL = 320
SLOTS = 20
MSG = LV * ROWS
WIDE = 56
ZROW = 25
F32, BF16 = jnp.float32, jnp.bfloat16
NT = (((1,), (1,)), ((), ()))
NN = (((1,), (0,)), ((), ()))
HIGH = lax.Precision.HIGHEST


def own_slot(b):
    return 5 * (b >> 2) + (b & 3)


def shared_slot(b):
    return 5 * (b >> 2) + 4


def call(kernel, out_shape, in_specs, scratch, flops=10**7):
    many = isinstance(out_shape, (tuple, list))
    vm = pl.BlockSpec(memory_space=pltpu.VMEM)
    return pl.pallas_call(
        kernel,
        out_shape=out_shape,
        in_specs=in_specs,
        out_specs=[vm] * len(out_shape) if many else vm,
        scratch_shapes=scratch,
        interpret=INTERPRET,
        cost_estimate=pl.CostEstimate(flops=flops, bytes_accessed=10**6, transcendentals=0),
    )


VM = pl.BlockSpec(memory_space=pltpu.VMEM)
ANY = pl.BlockSpec(memory_space=pl.ANY)
SM = pl.BlockSpec(memory_space=pltpu.SMEM)


def cos_sin(phase):
    quad = jnp.floor((phase + 160.5) * (1.0 / 320.0))
    x = (phase - 320.0 * quad) * (2.0 * math.pi / NLON)
    z = x * x
    s = x * (1.0 + z * (-1.6666654611e-1 + z * (8.3321608736e-3 - z * 1.9515295891e-4)))
    c = 1.0 - 0.5 * z + z * z * (
        4.166664568298827e-2 + z * (-1.388731625493765e-3 + z * 2.443315711809948e-5)
    )
    odd = jnp.logical_or(quad == 1.0, quad == 3.0)
    c, s = jnp.where(odd, s, c), jnp.where(odd, c, s)
    c = jnp.where(jnp.logical_or(quad == 1.0, quad == 2.0), -c, c)
    s = jnp.where(jnp.logical_or(quad == 2.0, quad == 3.0), -s, s)
    return c, s


def wrapped(count):
    return count - NLON * jnp.floor((count + 0.5) * (1.0 / NLON))


CHUNK = 64


def tables_kernel(assign_ref, t_out, even_ref, weight_ref, t_ref, sems):
    def write(i):
        rows = pl.ds(pl.multiple_of(i * CHUNK, CHUNK), CHUNK)
        return pltpu.make_async_copy(t_ref.at[:, rows], t_out.at[:, rows], sems.at[i])

    slots = lax.broadcasted_iota(jnp.int32, (CHUNK, M), 1)
    lane = lax.broadcasted_iota(jnp.int32, (CHUNK, 128), 1)
    lane_f = lane.astype(F32)
    assign = assign_ref[...].reshape(1, M).astype(F32)

    def step(i, carry):
        r0 = pl.multiple_of(i * CHUNK, CHUNK)
        d = r0 + lax.broadcasted_iota(jnp.int32, (CHUNK, 1), 0)
        lev = d & 15
        waves, evens, weights = [], [], []
        for slot in (own_slot(lev), shared_slot(lev)):
            wave = jnp.sum(jnp.where(slots == (d >> 4) * SLOTS + slot, assign, 0.0), axis=1, keepdims=True)
            waves.append(wave)
            evens.append(jnp.where(wave == 2.0 * jnp.floor(wave * 0.5), 1.0, 0.0))
            weights.append(jnp.where(wave == 0.0, 1.0, 2.0))
        turn_c, turn_s = cos_sin(wrapped(jnp.where(lane == 0, waves[0], waves[1]) * 128.0))

        def put(j, block, value):
            high = value.astype(BF16)
            t_ref[j, pl.ds(r0, CHUNK), 128 * block : 128 * block + 128] = high
            low = (value - high.astype(F32)).astype(BF16)
            t_ref[j, pl.ds(r0, CHUNK), HALF_LON + 128 * block : HALF_LON + 128 * block + 128] = low

        for u in range(2):
            start = wrapped(waves[u] * lane_f + (jnp.where((lev & 2) == 2, 320.0, 0.0) if u else 0.0))
            c, s = cos_sin(start)
            c = c * (1.0 / math.sqrt(NLON))
            s = s * (1.0 / math.sqrt(NLON))
            cd, sd = turn_c[:, u : u + 1], turn_s[:, u : u + 1]
            for block in range(5):
                put(2 * u, block, c)
                if u == 0:
                    put(1, block, -s)
                if block < 4:
                    c, s = c * cd - s * sd, s * cd + c * sd
        even_ref[pl.ds(r0, CHUNK), :] = jnp.where(
            lane < 2 * MSG, evens[0], evens[1]
        )
        weight_ref[pl.ds(r0, CHUNK), :] = jnp.where(
            lane < 2 * MSG, weights[0], weights[1]
        )
        write(i).start()
        return carry

    lax.fori_loop(0, N_DEV // CHUNK, step, 0)
    for i in range(N_DEV // CHUNK):
        write(i).wait()


def tables(assign):
    return pl.pallas_call(
        tables_kernel,
        out_shape=(
            jax.ShapeDtypeStruct((3, N_DEV, NLON), BF16),
            jax.ShapeDtypeStruct((N_DEV, 128), F32),
            jax.ShapeDtypeStruct((N_DEV, 128), F32),
        ),
        in_specs=[VM],
        out_specs=(ANY, VM, VM),
        scratch_shapes=[pltpu.VMEM((3, N_DEV, NLON), BF16), pltpu.SemaphoreType.DMA((N_DEV // CHUNK,))],
        name="tables",
        interpret=INTERPRET,
        cost_estimate=pl.CostEstimate(flops=10**7, bytes_accessed=10**6, transcendentals=0),
    )(assign)


def forward_kernel(
    side_ref,
    stencil_ref,
    tracer_ref,
    near_ref,
    far_ref,
    off_ref,
    t_any,
    even_ref,
    out_ref,
    pad,
    rolled,
    codes,
    adv,
    fe,
    fo,
    t_ref,
    t_sem,
):
    fetch = pltpu.make_async_copy(t_any, t_ref, t_sem)
    fetch.start()
    odd_band = side_ref[0] == 1
    pad[...] = jnp.zeros((64, NLON), F32)
    for i in range(3):
        pad[2 + 2 * i : 4 + 2 * i, :] = jnp.where(odd_band, near_ref[i], far_ref[i])
        pad[48 + 2 * i : 50 + 2 * i, :] = jnp.where(odd_band, far_ref[i], near_ref[i])
    for i in range(ROWS):
        pad[8 + 2 * i : 10 + 2 * i, :] = tracer_ref[i]
        codes[2 * i : 2 * i + 2, :] = off_ref[i]
    for bi in range(7):
        shift = (3 - bi) % NLON
        rolled[bi] = pltpu.roll(pad[...], shift, 1) if shift else pad[...]

    first = (lax.broadcasted_iota(jnp.int32, (2 * ROWS, 128), 0) & 1) == 0

    def chunk(ci, carry):
        l0 = pl.multiple_of(ci * 128, 128)
        value = codes[:, pl.ds(l0, 128)]
        part = jnp.where(first, value * 7, value)
        code = part + jnp.where(first, jnp.roll(part, -1, 0), jnp.roll(part, 1, 0))
        acc = jnp.zeros((2 * ROWS, 128), F32)
        for ai in range(7):
            for bi in range(7):
                s = stencil_ref[ai, bi]
                w = jnp.where(code == (ai - 3) * 7 + (bi - 3), s + 1.0, s)
                acc = acc + w * rolled[bi, 2 + 2 * ai : 42 + 2 * ai, pl.ds(l0, 128)]
        adv[ci] = acc
        return carry

    lax.fori_loop(0, NLON // 128, chunk, 0)
    levels = [
        jnp.concatenate([every_other(adv, ci, k) for ci in range(NLON // 128)], axis=1) for k in range(LV)
    ]
    x = jnp.concatenate(
        [v[:, :HALF_LON] + v[:, HALF_LON:] for v in levels] + [v[:, :HALF_LON] - v[:, HALF_LON:] for v in levels], axis=0
    )
    high = x.astype(BF16)
    low = (x - high.astype(F32)).astype(BF16)
    right = jnp.concatenate(
        [
            jnp.concatenate([high, high], axis=1),
            jnp.concatenate([low, jnp.zeros_like(low)], axis=1),
        ],
        axis=0,
    )
    fe[...] = jnp.zeros((N_DEV, 128), F32)
    fo[...] = jnp.zeros((N_DEV, 128), F32)
    fetch.wait()
    for j in range(3):
        prod = lax.dot_general(t_ref[j], right, NT, preferred_element_type=F32)
        fe[:, MSG * j : MSG * (j + 1)] = prod[:, 0:MSG] + prod[:, 2 * MSG : 3 * MSG]
        fo[:, MSG * j : MSG * (j + 1)] = prod[:, MSG : 2 * MSG] + prod[:, 3 * MSG : 4 * MSG]
    out_ref[...] = jnp.where(even_ref[...] > 0.5, fe[...], fo[...])


def every_other(ref, ci, k):
    return ref[ci][k::2] if INTERPRET else ref[ci, pl.ds(k, ROWS, 2), :]


def forward(side, stencil, tracer, near, far, offsets, table, even):
    return call(
        forward_kernel,
        jax.ShapeDtypeStruct((N_DEV, 128), F32),
        [SM, SM, VM, VM, VM, VM, ANY, VM],
        [
            pltpu.VMEM((64, NLON), F32),
            pltpu.VMEM((7, 64, NLON), F32),
            pltpu.VMEM((2 * ROWS, NLON), jnp.int32),
            pltpu.VMEM((NLON // 128, 2 * ROWS, 128), F32),
            pltpu.VMEM((N_DEV, 128), F32),
            pltpu.VMEM((N_DEV, 128), F32),
            pltpu.VMEM((3, N_DEV, NLON), BF16),
            pltpu.SemaphoreType.DMA,
        ],
        10**9,
    )(side, stencil, tracer, near, far, offsets, table, even)


def mirror_matrix():
    src = lax.broadcasted_iota(jnp.int32, (128, 128), 0)
    dst = lax.broadcasted_iota(jnp.int32, (128, 128), 1)
    hit = jnp.zeros((128, 128), jnp.bool_)
    for g in range(6):
        hit = jnp.logical_or(
            hit, jnp.logical_and(jnp.logical_and(dst >= 20 * g, dst < 20 * g + 20), src + dst == 40 * g + 19)
        )
    return hit.astype(F32)


def spectral_kernel(
    lat_ref,
    lev_ref,
    assign_ref,
    msg_ref,
    own_ref,
    shared_ref,
    damping_ref,
    inv_in,
    vec_in,
    out_ref,
    nbuf,
    sbuf,
    flip,
    zonal,
    wide,
):
    mirror = mirror_matrix()
    half = N_DEV // 2
    flip[...] = lax.dot_general(msg_ref[half:, :], mirror, NN, precision=HIGH, preferred_element_type=F32)
    for a in range(N_LAT // 2):
        top = msg_ref[16 * a : 16 * a + 16, :]
        low = flip[16 * (15 - a) : 16 * (15 - a) + 16, :]
        for j in range(3):
            for k in range(LV):
                lane = MSG * j + ROWS * k
                nbuf[j, 16 * k : 16 * k + 16, ROWS * a : ROWS * a + ROWS] = top[:, lane : lane + ROWS]
                sbuf[j, 16 * k : 16 * k + 16, ROWS * a : ROWS * a + ROWS] = low[:, lane : lane + ROWS]

    def exact(left, right):
        return lax.dot_general(left, right, NN, precision=HIGH, preferred_element_type=F32)

    lev = lev_ref[0]
    base = lat_ref[0] * SLOTS
    own_wave = assign_ref[base + own_slot(lev)]
    shared_wave = assign_ref[base + shared_slot(lev)]
    row = lax.broadcasted_iota(jnp.int32, (NLEV, NLEV), 0)
    column = lax.broadcasted_iota(jnp.int32, (NLEV, NLEV), 1)
    damp = jnp.sum(jnp.where(row == column, damping_ref[...].reshape(1, NLEV), 0.0), axis=1, keepdims=True)
    levels = (row == 2 * (column & 15) + (column >> 4)).astype(F32)
    places = (column == 2 * (row & 15) + (row >> 4)).astype(F32)
    inv_one = exact(inv_in[...], levels)
    vec_one = vec_in[...]
    vecp_one = exact(places, vec_one)

    def blocks(matrix, count):
        if count == 1:
            return matrix
        zero = jnp.zeros_like(matrix)
        return jnp.concatenate(
            [jnp.concatenate([matrix, zero], axis=1), jnp.concatenate([zero, matrix], axis=1)], axis=0
        )

    def solve(units, matrix, degree, odd):
        count = len(units)
        hemi = jnp.concatenate(
            [part for j in units for part in (nbuf[j] + sbuf[j], nbuf[j] - sbuf[j])], axis=0
        ).astype(BF16)
        prod = lax.dot_general(hemi, matrix, NT, preferred_element_type=F32)
        keep = degree <= M - 1
        forcing = jnp.concatenate(
            [
                jnp.where(keep, jnp.where(odd, prod[64 * u + 32 : 64 * u + 64], prod[64 * u : 64 * u + 32]), 0.0)
                for u in range(count)
            ],
            axis=0,
        )
        n = degree.astype(F32)
        denominator = 1.0 + (n * (n + 1.0) / float(M * M)) * damp
        modal = exact(blocks(inv_one, count), forcing)
        modal = jnp.concatenate([modal[32 * u : 32 * u + 32] / denominator for u in range(count)], axis=0)
        packed = exact(blocks(vecp_one, count), modal)
        left = jnp.concatenate(
            [
                part
                for u in range(count)
                for part in (
                    packed[32 * u : 32 * u + 32],
                    jnp.where(odd, -packed[32 * u : 32 * u + 32], packed[32 * u : 32 * u + 32]),
                )
            ],
            axis=0,
        ).astype(BF16)
        back = lax.dot_general(left, matrix, NN, preferred_element_type=F32)
        for u, j in enumerate(units):
            lats = jnp.concatenate([back[64 * u : 64 * u + 32], back[64 * u + 32 : 64 * u + 64]], axis=1)
            for tile in range(5):
                zonal[tile, 32 * j : 32 * j + 32, :] = lats[:, 128 * tile : 128 * tile + 128]
        return exact(blocks(vec_one, count), modal).T

    lane = lax.broadcasted_iota(jnp.int32, (32, QP), 1)
    whole = solve((0, 1), own_ref[...], lane + own_wave, (lane & 1) == 1)
    lane = lax.broadcasted_iota(jnp.int32, (32, QP // 2), 1)
    block = jnp.floor((lane.astype(F32) + 0.5) * (1.0 / 20.0)).astype(jnp.int32)
    part = solve((2,), shared_ref[...], lane + 20 * block + 20 * (lev & 1) + shared_wave, (lane & 1) == 1)
    for b in range(N_LEV):
        wide[b, 0:20, 0:64] = whole[QB * b : QB * b + 20]
        wide[b, 0:20, 64:128] = whole[QB * b + 20 : QB * b + 40]
        for g in range(4):
            wide[b, 20:25, 32 * g : 32 * g + 32] = part[20 * b + 5 * g : 20 * b + 5 * g + 5]
        for tile in range(5):
            wide[b, ZROW + 6 * tile : ZROW + 6 * tile + 6, :] = strided(zonal, tile, b, 6, 16)
        wide[b, ZROW + 30 : WIDE, :] = jnp.zeros((WIDE - ZROW - 30, 128), F32)
    out_ref[...] = wide[...].astype(BF16)


def strided(ref, tile, start, count, stride):
    if INTERPRET:
        return ref[tile][start :: stride][:count]
    return ref[tile, pl.ds(start, count, stride), :]


def spectral(lat, lev, assign, msgs, own, shared, damping, inv, vec):
    return call(
        spectral_kernel,
        jax.ShapeDtypeStruct((N_LEV, WIDE, 128), BF16),
        [SM, SM, SM, VM, VM, VM, VM, VM, VM],
        [
            pltpu.VMEM((3, 32, HL), F32),
            pltpu.VMEM((3, 32, HL), F32),
            pltpu.VMEM((N_DEV // 2, 128), F32),
            pltpu.VMEM((5, 96, 128), F32),
            pltpu.VMEM((N_LEV, WIDE, 128), F32),
        ],
        10**9,
    )(lat, lev, assign, msgs, own, shared, damping, inv, vec)


def bands_kernel(wide_ref, out_ref, rows, out, flip):
    half = N_DEV // 2
    for b in range(N_LEV):
        value = wide_ref[b].astype(F32)
        for tile in range(5):
            rows[tile, 8 * b : 8 * b + 6, :] = value[ZROW + 6 * tile : ZROW + 6 * tile + 6]
    out[...] = jnp.zeros((half, 128), F32)
    flip[...] = jnp.zeros((half, 128), F32)
    for j in range(3):
        for k in range(LV):
            lane = MSG * j + ROWS * k
            lats = jnp.concatenate([strided(rows, tile, LV * j + k, N_LEV, 8) for tile in range(5)], axis=1)
            for a in range(N_LAT // 2):
                out[16 * a : 16 * a + 16, lane : lane + ROWS] = lats[:, ROWS * a : ROWS * a + ROWS]
                flip[16 * (15 - a) : 16 * (15 - a) + 16, lane : lane + ROWS] = lats[:, HL + ROWS * a : HL + ROWS * a + ROWS]
    mirror = mirror_matrix().astype(BF16)
    low = lax.dot_general(flip[...].astype(BF16), mirror, NN, preferred_element_type=F32)
    out_ref[:half, :] = out[...].astype(BF16)
    out_ref[half:, :] = low.astype(BF16)


def bands(wide):
    return call(
        bands_kernel,
        jax.ShapeDtypeStruct((N_DEV, 128), BF16),
        [VM],
        [
            pltpu.VMEM((5, 8 * N_LEV, 128), F32),
            pltpu.VMEM((N_DEV // 2, 128), F32),
            pltpu.VMEM((N_DEV // 2, 128), F32),
        ],
        10**7,
    )(wide)


def inverse_kernel(msg_ref, t_any, even_ref, weight_ref, out_ref, t_ref, t_sem):
    fetches = [
        pltpu.make_async_copy(t_any.at[j, :, pl.ds(0, HALF_LON)], t_ref.at[j], t_sem.at[j]) for j in range(3)
    ]
    for fetch in fetches:
        fetch.start()
    lane = lax.broadcasted_iota(jnp.int32, (N_DEV, 128), 1)
    scaled = jnp.where(lane < 3 * MSG, msg_ref[...].astype(F32) * weight_ref[...], 0.0)
    even = (scaled * even_ref[...]).T
    odd = (scaled * (1.0 - even_ref[...])).T
    total = jnp.zeros((2 * MSG, HALF_LON), F32)
    for j in range(3):
        fetches[j].wait()
        left = jnp.concatenate([even[MSG * j : MSG * (j + 1)], odd[MSG * j : MSG * (j + 1)]], axis=0).astype(BF16)
        total = total + lax.dot_general(left, t_ref[j], NN, preferred_element_type=F32)
    near = total[:MSG] + total[MSG:]
    far = total[:MSG] - total[MSG:]
    for k in range(LV):
        out_ref[:, k, :HALF_LON] = near[ROWS * k : ROWS * (k + 1)]
        out_ref[:, k, HALF_LON:] = far[ROWS * k : ROWS * (k + 1)]


def inverse(msgs, table, even, weight):
    return call(
        inverse_kernel,
        jax.ShapeDtypeStruct((ROWS, LV, NLON), F32),
        [VM, ANY, VM, VM],
        [pltpu.VMEM((3, N_DEV, HALF_LON), BF16), pltpu.SemaphoreType.DMA((3,))],
        10**8,
    )(msgs, table, even, weight)


def place_kernel(spec_ref, out_ref):
    for b in range(N_LEV):
        c, half = (b & 3) >> 1, b & 1
        value = spec_ref[b].astype(F32)
        out_ref[own_slot(b), 0:20, :] = value[0:20, 0:64]
        out_ref[own_slot(b), 20:40, :] = value[0:20, 64:128]
        for g in range(4):
            first = 20 * half + 5 * g
            out_ref[shared_slot(b), first : first + 5, 32 * c : 32 * c + 32] = value[20:25, 32 * g : 32 * g + 32]


def place(spec):
    return call(place_kernel, jax.ShapeDtypeStruct((SLOTS, QB, 64), F32), [VM], [], 10**6)(spec)


def send_kernel(table_ref, out_ref, sems):
    copies = []
    for b in range(N_LEV):
        copies.append(pltpu.make_async_copy(table_ref.at[own_slot(b)], out_ref.at[b, pl.ds(0, 20)], sems.at[2 * b]))
        half = table_ref.at[shared_slot(b), pl.ds(10 * (b & 1), 10)]
        copies.append(pltpu.make_async_copy(half, out_ref.at[b, pl.ds(20, 10)], sems.at[2 * b + 1]))
    for copy in copies:
        copy.start()
    for copy in copies:
        copy.wait()


def send_tables(legendre):
    return pl.pallas_call(
        send_kernel,
        out_shape=jax.ShapeDtypeStruct((N_LEV, 30, 2, HL), BF16),
        in_specs=[VM],
        out_specs=ANY,
        scratch_shapes=[pltpu.SemaphoreType.DMA((2 * N_LEV,))],
        name="send_tables",
        interpret=INTERPRET,
        cost_estimate=pl.CostEstimate(flops=10**6, bytes_accessed=2 * 10**6, transcendentals=0),
    )(jnp.swapaxes(legendre, 1, 2))


def received_tables(got):
    return got[:, :20].reshape(QP, HL), got[:, 20:].reshape(QP // 2, HL)


def exchange(value, axes):
    return lax.all_to_all(value, axes, split_axis=0, concat_axis=0, tiled=True)


def step_of(tracer, offsets, stencil, assign, legendre, damping, vert_vecs, vert_inv):
    lat = lax.axis_index("lat")
    side = lat & 1
    rows = jnp.swapaxes(tracer, 0, 1)
    near = lax.dynamic_slice_in_dim(rows, jnp.where(side == 1, 0, ROWS - 3), 3)
    near = lax.ppermute(near, "lat", [(i, i ^ 1) for i in range(N_LAT)])
    far = lax.dynamic_slice_in_dim(rows, jnp.where(side == 1, ROWS - 3, 0), 3)
    far = lax.ppermute(far, "lat", [(i, i + 2 * (i & 1) - 1) for i in range(1, N_LAT - 1)])
    table, even, weight = tables(assign)
    packed = send_tables(legendre)
    matrices = exchange(packed, "lev")
    own, shared = received_tables(matrices)
    msgs = forward(side.reshape(1), stencil, rows, near, far, jnp.swapaxes(offsets, 0, 1), table, even)
    got = exchange(msgs.reshape(N_DEV, 1, 128), ("lat", "lev")).reshape(N_DEV, 128)
    lev = lax.axis_index("lev")
    solved = spectral(
        lat.astype(jnp.int32).reshape(1),
        lev.astype(jnp.int32).reshape(1),
        assign,
        got,
        own,
        shared,
        damping,
        vert_inv,
        vert_vecs,
    )
    solved = exchange(solved, "lev")
    home = exchange(bands(solved).reshape(N_LAT, N_LEV, 128), "lat").reshape(N_DEV, 128)
    tracer_new = inverse(home, table, even, weight)
    spectral_new = place(solved).reshape(SLOTS, 20, 2, 64)
    return jnp.swapaxes(tracer_new, 0, 1), jnp.swapaxes(spectral_new, 1, 2)


def solution(mesh):
    placed = (
        P("lev", "lat", None),
        P(None, "lat", None),
        P(),
        P(),
        P("lat", None, "lev", None),
        P(),
        P(),
        P(),
    )
    return jax.shard_map(
        step_of,
        mesh=mesh,
        in_specs=placed,
        out_specs=(P("lev", "lat", None), P("lat", None, "lev", None)),
        check_vma=False,
    )
```

```python
import math

import jax
import jax.numpy as jnp
from jax import lax
from jax.experimental import pallas as pl
from jax.experimental.pallas import tpu as pltpu
from jax.sharding import PartitionSpec as P


INTERPRET = False
N_LAT, N_LEV = 32, 16
N_DEV = N_LAT * N_LEV
M = 640
NLON, HALF_LON = 1280, 640
ROWS = 20
LV = 2
NLEV = 32
QB = 40
QP = N_LEV * QB
HL = 320
SLOTS = 20
MSG = LV * ROWS
WIDE = 56
ZROW = 25
F32, BF16 = jnp.float32, jnp.bfloat16
NT = (((1,), (1,)), ((), ()))
NN = (((1,), (0,)), ((), ()))
HIGH = lax.Precision.HIGHEST


def own_slot(b):
    return 5 * (b >> 2) + (b & 3)


def shared_slot(b):
    return 5 * (b >> 2) + 4


def call(kernel, out_shape, in_specs, scratch, flops=10**7):
    many = isinstance(out_shape, (tuple, list))
    vm = pl.BlockSpec(memory_space=pltpu.VMEM)
    return pl.pallas_call(
        kernel,
        out_shape=out_shape,
        in_specs=in_specs,
        out_specs=[vm] * len(out_shape) if many else vm,
        scratch_shapes=scratch,
        interpret=INTERPRET,
        cost_estimate=pl.CostEstimate(flops=flops, bytes_accessed=10**6, transcendentals=0),
    )


VM = pl.BlockSpec(memory_space=pltpu.VMEM)
ANY = pl.BlockSpec(memory_space=pl.ANY)
SM = pl.BlockSpec(memory_space=pltpu.SMEM)


def cos_sin(phase):
    quad = jnp.floor((phase + 160.5) * (1.0 / 320.0))
    x = (phase - 320.0 * quad) * (2.0 * math.pi / NLON)
    z = x * x
    s = x * (1.0 + z * (-1.6666654611e-1 + z * (8.3321608736e-3 - z * 1.9515295891e-4)))
    c = 1.0 - 0.5 * z + z * z * (
        4.166664568298827e-2 + z * (-1.388731625493765e-3 + z * 2.443315711809948e-5)
    )
    odd = jnp.logical_or(quad == 1.0, quad == 3.0)
    c, s = jnp.where(odd, s, c), jnp.where(odd, c, s)
    c = jnp.where(jnp.logical_or(quad == 1.0, quad == 2.0), -c, c)
    s = jnp.where(jnp.logical_or(quad == 2.0, quad == 3.0), -s, s)
    return c, s


def wrapped(count):
    return count - NLON * jnp.floor((count + 0.5) * (1.0 / NLON))


CHUNK = 64


def tables_kernel(assign_ref, t_out, even_ref, weight_ref, t_ref, sems):
    def write(i):
        rows = pl.ds(pl.multiple_of(i * CHUNK, CHUNK), CHUNK)
        return pltpu.make_async_copy(t_ref.at[:, rows], t_out.at[:, rows], sems.at[i])

    slots = lax.broadcasted_iota(jnp.int32, (CHUNK, M), 1)
    lane = lax.broadcasted_iota(jnp.int32, (CHUNK, 128), 1)
    lane_f = lane.astype(F32)
    assign = assign_ref[...].reshape(1, M).astype(F32)

    def step(i, carry):
        r0 = pl.multiple_of(i * CHUNK, CHUNK)
        d = r0 + lax.broadcasted_iota(jnp.int32, (CHUNK, 1), 0)
        lev = d & 15
        waves, evens, weights = [], [], []
        for slot in (own_slot(lev), shared_slot(lev)):
            wave = jnp.sum(jnp.where(slots == (d >> 4) * SLOTS + slot, assign, 0.0), axis=1, keepdims=True)
            waves.append(wave)
            evens.append(jnp.where(wave == 2.0 * jnp.floor(wave * 0.5), 1.0, 0.0))
            weights.append(jnp.where(wave == 0.0, 1.0, 2.0))
        turn_c, turn_s = cos_sin(wrapped(jnp.where(lane == 0, waves[0], waves[1]) * 128.0))

        def put(j, block, value):
            high = value.astype(BF16)
            t_ref[j, pl.ds(r0, CHUNK), 128 * block : 128 * block + 128] = high
            low = (value - high.astype(F32)).astype(BF16)
            t_ref[j, pl.ds(r0, CHUNK), HALF_LON + 128 * block : HALF_LON + 128 * block + 128] = low

        for u in range(2):
            start = wrapped(waves[u] * lane_f + (jnp.where((lev & 2) == 2, 320.0, 0.0) if u else 0.0))
            c, s = cos_sin(start)
            c = c * (1.0 / math.sqrt(NLON))
            s = s * (1.0 / math.sqrt(NLON))
            cd, sd = turn_c[:, u : u + 1], turn_s[:, u : u + 1]
            for block in range(5):
                put(2 * u, block, c)
                if u == 0:
                    put(1, block, -s)
                if block < 4:
                    c, s = c * cd - s * sd, s * cd + c * sd
        even_ref[pl.ds(r0, CHUNK), :] = jnp.where(
            lane < 2 * MSG, evens[0], evens[1]
        )
        weight_ref[pl.ds(r0, CHUNK), :] = jnp.where(
            lane < 2 * MSG, weights[0], weights[1]
        )
        write(i).start()
        return carry

    lax.fori_loop(0, N_DEV // CHUNK, step, 0)
    for i in range(N_DEV // CHUNK):
        write(i).wait()


def tables(assign):
    return pl.pallas_call(
        tables_kernel,
        out_shape=(
            jax.ShapeDtypeStruct((3, N_DEV, NLON), BF16),
            jax.ShapeDtypeStruct((N_DEV, 128), F32),
            jax.ShapeDtypeStruct((N_DEV, 128), F32),
        ),
        in_specs=[VM],
        out_specs=(ANY, VM, VM),
        scratch_shapes=[pltpu.VMEM((3, N_DEV, NLON), BF16), pltpu.SemaphoreType.DMA((N_DEV // CHUNK,))],
        name="tables",
        interpret=INTERPRET,
        cost_estimate=pl.CostEstimate(flops=10**7, bytes_accessed=10**6, transcendentals=0),
    )(assign)


def forward_kernel(
    side_ref,
    stencil_ref,
    tracer_ref,
    near_ref,
    far_ref,
    off_ref,
    t_any,
    even_ref,
    out_ref,
    pad,
    rolled,
    codes,
    adv,
    fe,
    fo,
    t_ref,
    t_sem,
):
    fetch = pltpu.make_async_copy(t_any, t_ref, t_sem)
    fetch.start()
    odd_band = side_ref[0] == 1
    pad[...] = jnp.zeros((64, NLON), F32)
    for i in range(3):
        pad[2 + 2 * i : 4 + 2 * i, :] = jnp.where(odd_band, near_ref[i], far_ref[i])
        pad[48 + 2 * i : 50 + 2 * i, :] = jnp.where(odd_band, far_ref[i], near_ref[i])
    for i in range(ROWS):
        pad[8 + 2 * i : 10 + 2 * i, :] = tracer_ref[i]
        codes[2 * i : 2 * i + 2, :] = off_ref[i]
    for bi in range(7):
        shift = (3 - bi) % NLON
        rolled[bi] = pltpu.roll(pad[...], shift, 1) if shift else pad[...]

    first = (lax.broadcasted_iota(jnp.int32, (2 * ROWS, 128), 0) & 1) == 0

    def chunk(ci, carry):
        l0 = pl.multiple_of(ci * 128, 128)
        value = codes[:, pl.ds(l0, 128)]
        part = jnp.where(first, value * 7, value)
        code = part + jnp.where(first, jnp.roll(part, -1, 0), jnp.roll(part, 1, 0))
        acc = jnp.zeros((2 * ROWS, 128), F32)
        for ai in range(7):
            for bi in range(7):
                s = stencil_ref[ai, bi]
                w = jnp.where(code == (ai - 3) * 7 + (bi - 3), s + 1.0, s)
                acc = acc + w * rolled[bi, 2 + 2 * ai : 42 + 2 * ai, pl.ds(l0, 128)]
        adv[ci] = acc
        return carry

    lax.fori_loop(0, NLON // 128, chunk, 0)
    levels = [
        jnp.concatenate([every_other(adv, ci, k) for ci in range(NLON // 128)], axis=1) for k in range(LV)
    ]
    x = jnp.concatenate(
        [v[:, :HALF_LON] + v[:, HALF_LON:] for v in levels] + [v[:, :HALF_LON] - v[:, HALF_LON:] for v in levels], axis=0
    )
    high = x.astype(BF16)
    low = (x - high.astype(F32)).astype(BF16)
    right = jnp.concatenate(
        [
            jnp.concatenate([high, high], axis=1),
            jnp.concatenate([low, jnp.zeros_like(low)], axis=1),
        ],
        axis=0,
    )
    fe[...] = jnp.zeros((N_DEV, 128), F32)
    fo[...] = jnp.zeros((N_DEV, 128), F32)
    fetch.wait()
    for j in range(3):
        prod = lax.dot_general(t_ref[j], right, NT, preferred_element_type=F32)
        fe[:, MSG * j : MSG * (j + 1)] = prod[:, 0:MSG] + prod[:, 2 * MSG : 3 * MSG]
        fo[:, MSG * j : MSG * (j + 1)] = prod[:, MSG : 2 * MSG] + prod[:, 3 * MSG : 4 * MSG]
    out_ref[...] = jnp.where(even_ref[...] > 0.5, fe[...], fo[...])


def every_other(ref, ci, k):
    return ref[ci][k::2] if INTERPRET else ref[ci, pl.ds(k, ROWS, 2), :]


def forward(side, stencil, tracer, near, far, offsets, table, even):
    return call(
        forward_kernel,
        jax.ShapeDtypeStruct((N_DEV, 128), F32),
        [SM, SM, VM, VM, VM, VM, ANY, VM],
        [
            pltpu.VMEM((64, NLON), F32),
            pltpu.VMEM((7, 64, NLON), F32),
            pltpu.VMEM((2 * ROWS, NLON), jnp.int32),
            pltpu.VMEM((NLON // 128, 2 * ROWS, 128), F32),
            pltpu.VMEM((N_DEV, 128), F32),
            pltpu.VMEM((N_DEV, 128), F32),
            pltpu.VMEM((3, N_DEV, NLON), BF16),
            pltpu.SemaphoreType.DMA,
        ],
        10**9,
    )(side, stencil, tracer, near, far, offsets, table, even)


def mirror_matrix():
    src = lax.broadcasted_iota(jnp.int32, (128, 128), 0)
    dst = lax.broadcasted_iota(jnp.int32, (128, 128), 1)
    hit = jnp.zeros((128, 128), jnp.bool_)
    for g in range(6):
        hit = jnp.logical_or(
            hit, jnp.logical_and(jnp.logical_and(dst >= 20 * g, dst < 20 * g + 20), src + dst == 40 * g + 19)
        )
    return hit.astype(F32)


def spectral_kernel(
    lat_ref,
    lev_ref,
    assign_ref,
    msg_ref,
    own_ref,
    shared_ref,
    damping_ref,
    inv_in,
    vec_in,
    out_ref,
    nbuf,
    sbuf,
    flip,
    zonal,
    wide,
):
    mirror = mirror_matrix()
    half = N_DEV // 2
    flip[...] = lax.dot_general(msg_ref[half:, :], mirror, NN, precision=HIGH, preferred_element_type=F32)
    for a in range(N_LAT // 2):
        top = msg_ref[16 * a : 16 * a + 16, :]
        low = flip[16 * (15 - a) : 16 * (15 - a) + 16, :]
        for j in range(3):
            for k in range(LV):
                lane = MSG * j + ROWS * k
                nbuf[j, 16 * k : 16 * k + 16, ROWS * a : ROWS * a + ROWS] = top[:, lane : lane + ROWS]
                sbuf[j, 16 * k : 16 * k + 16, ROWS * a : ROWS * a + ROWS] = low[:, lane : lane + ROWS]

    def exact(left, right):
        return lax.dot_general(left, right, NN, precision=HIGH, preferred_element_type=F32)

    lev = lev_ref[0]
    base = lat_ref[0] * SLOTS
    own_wave = assign_ref[base + own_slot(lev)]
    shared_wave = assign_ref[base + shared_slot(lev)]
    row = lax.broadcasted_iota(jnp.int32, (NLEV, NLEV), 0)
    column = lax.broadcasted_iota(jnp.int32, (NLEV, NLEV), 1)
    damp = jnp.sum(jnp.where(row == column, damping_ref[...].reshape(1, NLEV), 0.0), axis=1, keepdims=True)
    levels = (row == 2 * (column & 15) + (column >> 4)).astype(F32)
    places = (column == 2 * (row & 15) + (row >> 4)).astype(F32)
    inv_one = exact(inv_in[...], levels)
    vec_one = vec_in[...]
    vecp_one = exact(places, vec_one)

    def blocks(matrix, count):
        if count == 1:
            return matrix
        zero = jnp.zeros_like(matrix)
        return jnp.concatenate(
            [jnp.concatenate([matrix, zero], axis=1), jnp.concatenate([zero, matrix], axis=1)], axis=0
        )

    def solve(units, matrix, degree, odd):
        count = len(units)
        hemi = jnp.concatenate(
            [part for j in units for part in (nbuf[j] + sbuf[j], nbuf[j] - sbuf[j])], axis=0
        ).astype(BF16)
        prod = lax.dot_general(hemi, matrix, NT, preferred_element_type=F32)
        keep = degree <= M - 1
        forcing = jnp.concatenate(
            [
                jnp.where(keep, jnp.where(odd, prod[64 * u + 32 : 64 * u + 64], prod[64 * u : 64 * u + 32]), 0.0)
                for u in range(count)
            ],
            axis=0,
        )
        n = degree.astype(F32)
        denominator = 1.0 + (n * (n + 1.0) / float(M * M)) * damp
        modal = exact(blocks(inv_one, count), forcing)
        modal = jnp.concatenate([modal[32 * u : 32 * u + 32] / denominator for u in range(count)], axis=0)
        packed = exact(blocks(vecp_one, count), modal)
        left = jnp.concatenate(
            [
                part
                for u in range(count)
                for part in (
                    packed[32 * u : 32 * u + 32],
                    jnp.where(odd, -packed[32 * u : 32 * u + 32], packed[32 * u : 32 * u + 32]),
                )
            ],
            axis=0,
        ).astype(BF16)
        back = lax.dot_general(left, matrix, NN, preferred_element_type=F32)
        for u, j in enumerate(units):
            lats = jnp.concatenate([back[64 * u : 64 * u + 32], back[64 * u + 32 : 64 * u + 64]], axis=1)
            for tile in range(5):
                zonal[tile, 32 * j : 32 * j + 32, :] = lats[:, 128 * tile : 128 * tile + 128]
        return exact(blocks(vec_one, count), modal).T

    lane = lax.broadcasted_iota(jnp.int32, (32, QP), 1)
    whole = solve((0, 1), own_ref[...], lane + own_wave, (lane & 1) == 1)
    lane = lax.broadcasted_iota(jnp.int32, (32, QP // 2), 1)
    block = jnp.floor((lane.astype(F32) + 0.5) * (1.0 / 20.0)).astype(jnp.int32)
    part = solve((2,), shared_ref[...], lane + 20 * block + 20 * (lev & 1) + shared_wave, (lane & 1) == 1)
    for b in range(N_LEV):
        wide[b, 0:20, 0:64] = whole[QB * b : QB * b + 20]
        wide[b, 0:20, 64:128] = whole[QB * b + 20 : QB * b + 40]
        for g in range(4):
            wide[b, 20:25, 32 * g : 32 * g + 32] = part[20 * b + 5 * g : 20 * b + 5 * g + 5]
        for tile in range(5):
            wide[b, ZROW + 6 * tile : ZROW + 6 * tile + 6, :] = strided(zonal, tile, b, 6, 16)
        wide[b, ZROW + 30 : WIDE, :] = jnp.zeros((WIDE - ZROW - 30, 128), F32)
    out_ref[...] = wide[...].astype(BF16)


def strided(ref, tile, start, count, stride):
    if INTERPRET:
        return ref[tile][start :: stride][:count]
    return ref[tile, pl.ds(start, count, stride), :]


def spectral(lat, lev, assign, msgs, own, shared, damping, inv, vec):
    return call(
        spectral_kernel,
        jax.ShapeDtypeStruct((N_LEV, WIDE, 128), BF16),
        [SM, SM, SM, VM, VM, VM, VM, VM, VM],
        [
            pltpu.VMEM((3, 32, HL), F32),
            pltpu.VMEM((3, 32, HL), F32),
            pltpu.VMEM((N_DEV // 2, 128), F32),
            pltpu.VMEM((5, 96, 128), F32),
            pltpu.VMEM((N_LEV, WIDE, 128), F32),
        ],
        10**9,
    )(lat, lev, assign, msgs, own, shared, damping, inv, vec)


def bands_kernel(wide_ref, out_ref, rows, out, flip):
    half = N_DEV // 2
    for b in range(N_LEV):
        value = wide_ref[b].astype(F32)
        for tile in range(5):
            rows[tile, 8 * b : 8 * b + 6, :] = value[ZROW + 6 * tile : ZROW + 6 * tile + 6]
    out[...] = jnp.zeros((half, 128), F32)
    flip[...] = jnp.zeros((half, 128), F32)
    for j in range(3):
        for k in range(LV):
            lane = MSG * j + ROWS * k
            lats = jnp.concatenate([strided(rows, tile, LV * j + k, N_LEV, 8) for tile in range(5)], axis=1)
            for a in range(N_LAT // 2):
                out[16 * a : 16 * a + 16, lane : lane + ROWS] = lats[:, ROWS * a : ROWS * a + ROWS]
                flip[16 * (15 - a) : 16 * (15 - a) + 16, lane : lane + ROWS] = lats[:, HL + ROWS * a : HL + ROWS * a + ROWS]
    mirror = mirror_matrix().astype(BF16)
    low = lax.dot_general(flip[...].astype(BF16), mirror, NN, preferred_element_type=F32)
    out_ref[:half, :] = out[...].astype(BF16)
    out_ref[half:, :] = low.astype(BF16)


def bands(wide):
    return call(
        bands_kernel,
        jax.ShapeDtypeStruct((N_DEV, 128), BF16),
        [VM],
        [
            pltpu.VMEM((5, 8 * N_LEV, 128), F32),
            pltpu.VMEM((N_DEV // 2, 128), F32),
            pltpu.VMEM((N_DEV // 2, 128), F32),
        ],
        10**7,
    )(wide)


def inverse_kernel(msg_ref, t_any, even_ref, weight_ref, out_ref, t_ref, t_sem):
    fetches = [
        pltpu.make_async_copy(t_any.at[j, :, pl.ds(0, HALF_LON)], t_ref.at[j], t_sem.at[j]) for j in range(3)
    ]
    for fetch in fetches:
        fetch.start()
    lane = lax.broadcasted_iota(jnp.int32, (N_DEV, 128), 1)
    scaled = jnp.where(lane < 3 * MSG, msg_ref[...].astype(F32) * weight_ref[...], 0.0)
    even = (scaled * even_ref[...]).T
    odd = (scaled * (1.0 - even_ref[...])).T
    total = jnp.zeros((2 * MSG, HALF_LON), F32)
    for j in range(3):
        fetches[j].wait()
        left = jnp.concatenate([even[MSG * j : MSG * (j + 1)], odd[MSG * j : MSG * (j + 1)]], axis=0).astype(BF16)
        total = total + lax.dot_general(left, t_ref[j], NN, preferred_element_type=F32)
    near = total[:MSG] + total[MSG:]
    far = total[:MSG] - total[MSG:]
    for k in range(LV):
        out_ref[:, k, :HALF_LON] = near[ROWS * k : ROWS * (k + 1)]
        out_ref[:, k, HALF_LON:] = far[ROWS * k : ROWS * (k + 1)]


def inverse(msgs, table, even, weight):
    return call(
        inverse_kernel,
        jax.ShapeDtypeStruct((ROWS, LV, NLON), F32),
        [VM, ANY, VM, VM],
        [pltpu.VMEM((3, N_DEV, HALF_LON), BF16), pltpu.SemaphoreType.DMA((3,))],
        10**8,
    )(msgs, table, even, weight)


def place_kernel(spec_ref, out_ref):
    for b in range(N_LEV):
        c, half = (b & 3) >> 1, b & 1
        value = spec_ref[b].astype(F32)
        out_ref[own_slot(b), 0:20, :] = value[0:20, 0:64]
        out_ref[own_slot(b), 20:40, :] = value[0:20, 64:128]
        for g in range(4):
            first = 20 * half + 5 * g
            out_ref[shared_slot(b), first : first + 5, 32 * c : 32 * c + 32] = value[20:25, 32 * g : 32 * g + 32]


def place(spec):
    return call(place_kernel, jax.ShapeDtypeStruct((SLOTS, QB, 64), F32), [VM], [], 10**6)(spec)


def send_kernel(table_any, out_ref, table_ref, in_sems, sems):
    fetches = [pltpu.make_async_copy(table_any.at[r], table_ref.at[r], in_sems.at[r]) for r in range(SLOTS)]
    for fetch in fetches:
        fetch.start()
    copies = []
    for b in range(N_LEV):
        fetches[own_slot(b)].wait()
        copies.append(pltpu.make_async_copy(table_ref.at[own_slot(b)], out_ref.at[b, pl.ds(0, 20)], sems.at[2 * b]))
        copies[-1].start()
        if b & 3 == 3:
            fetches[shared_slot(b)].wait()
            for to in range(b - 3, b + 1):
                half = table_ref.at[shared_slot(b), pl.ds(10 * (to & 1), 10)]
                copies.append(pltpu.make_async_copy(half, out_ref.at[to, pl.ds(20, 10)], sems.at[2 * to + 1]))
                copies[-1].start()
    for copy in copies:
        copy.wait()


def send_tables(legendre):
    return pl.pallas_call(
        send_kernel,
        out_shape=jax.ShapeDtypeStruct((N_LEV, 30, 2, HL), BF16),
        in_specs=[ANY],
        out_specs=ANY,
        scratch_shapes=[
            pltpu.VMEM((SLOTS, 20, 2, HL), BF16),
            pltpu.SemaphoreType.DMA((SLOTS,)),
            pltpu.SemaphoreType.DMA((2 * N_LEV,)),
        ],
        name="send_tables",
        interpret=INTERPRET,
        cost_estimate=pl.CostEstimate(flops=10**6, bytes_accessed=2 * 10**6, transcendentals=0),
    )(jnp.swapaxes(legendre, 1, 2))


def received_tables(got):
    return got[:, :20].reshape(QP, HL), got[:, 20:].reshape(QP // 2, HL)


def exchange(value, axes):
    return lax.all_to_all(value, axes, split_axis=0, concat_axis=0, tiled=True)


def step_of(tracer, offsets, stencil, assign, legendre, damping, vert_vecs, vert_inv):
    lat = lax.axis_index("lat")
    side = lat & 1
    rows = jnp.swapaxes(tracer, 0, 1)
    near = lax.dynamic_slice_in_dim(rows, jnp.where(side == 1, 0, ROWS - 3), 3)
    near = lax.ppermute(near, "lat", [(i, i ^ 1) for i in range(N_LAT)])
    far = lax.dynamic_slice_in_dim(rows, jnp.where(side == 1, ROWS - 3, 0), 3)
    far = lax.ppermute(far, "lat", [(i, i + 2 * (i & 1) - 1) for i in range(1, N_LAT - 1)])
    table, even, weight = tables(assign)
    packed = send_tables(legendre)
    matrices = exchange(packed, "lev")
    own, shared = received_tables(matrices)
    msgs = forward(side.reshape(1), stencil, rows, near, far, jnp.swapaxes(offsets, 0, 1), table, even)
    got = exchange(msgs.reshape(N_DEV, 1, 128), ("lat", "lev")).reshape(N_DEV, 128)
    lev = lax.axis_index("lev")
    solved = spectral(
        lat.astype(jnp.int32).reshape(1),
        lev.astype(jnp.int32).reshape(1),
        assign,
        got,
        own,
        shared,
        damping,
        vert_inv,
        vert_vecs,
    )
    solved = exchange(solved, "lev")
    home = exchange(bands(solved).reshape(N_LAT, N_LEV, 128), "lat").reshape(N_DEV, 128)
    tracer_new = inverse(home, table, even, weight)
    spectral_new = place(solved).reshape(SLOTS, 20, 2, 64)
    return jnp.swapaxes(tracer_new, 0, 1), jnp.swapaxes(spectral_new, 1, 2)


def solution(mesh):
    placed = (
        P("lev", "lat", None),
        P(None, "lat", None),
        P(),
        P(),
        P("lat", None, "lev", None),
        P(),
        P(),
        P(),
    )
    return jax.shard_map(
        step_of,
        mesh=mesh,
        in_specs=placed,
        out_specs=(P("lev", "lat", None), P("lat", None, "lev", None)),
        check_vma=False,
    )
```
